32 devices in a mesh: dp: 32 (over z, y, x, core).
Axes of the slice: x: 2, y: 2, z: 4, core: 2. Of those that a mesh axis runs over, the one named last changes fastest.
Arguments:
- x_embed: bfloat16 [2048, 768], P('dp')
- positions: int32 [2048], P('dp')
- k_cache: bfloat16 [2, 2048, 32, 12, 64], P(None, 'dp')
- v_cache: bfloat16 [2, 2048, 32, 12, 64], P(None, 'dp')
- ln1_gain: bfloat16 [2, 768], P(None, 'dp')
- ln1_bias: bfloat16 [2, 768], P(None, 'dp')
- ln2_gain: bfloat16 [2, 768], P(None, 'dp')
- ln2_bias: bfloat16 [2, 768], P(None, 'dp')
- w_qkv: bfloat16 [2, 768, 2304], P(None, 'dp')
- b_qkv: bfloat16 [2, 2304], P(None, 'dp')
- w_out: bfloat16 [2, 768, 768], P(None, 'dp')
- b_out: bfloat16 [2, 768], P(None, 'dp')
- w_in: bfloat16 [2, 768, 3072], P(None, 'dp')
- b_in: bfloat16 [2, 3072], P(None, 'dp')
- w_down: bfloat16 [2, 3072, 768], P(None, 'dp')
- b_down: bfloat16 [2, 768], P(None, 'dp')
- lnf_gain: bfloat16 [768], P('dp')
- lnf_bias: bfloat16 [768], P('dp')
Outputs:
- output 1: bfloat16 [2048, 768], P('dp')
- output 2: bfloat16 [2, 2048, 32, 12, 64], P(None, 'dp')
- output 3: bfloat16 [2, 2048, 32, 12, 64], P(None, 'dp')
All inputs are finite; a program needn't handle non-finite values.
Results may differ from the reference program's by a relative error of at most 0.0109312.
Values are sent between devices in bfloat16 or wider.
A program may use at most 1 GiB of HBM per device.

```python
import jax
import jax.numpy as jnp
from jax import lax

LAYERS = 2
BATCH = 2048
SMAX = 32
D = 768
HEADS = 12
FF = 3072
HEAD = 64
ROT = 16

LN_EPS = 1e-5
ROPE_BASE = 10000.0


def setup_inputs(seed: int = 0) -> dict:
    root_key = jax.random.key(seed)
    subkeys = jax.random.split(root_key, 20)

    def normal(key_idx, arr_shape, std_dev):
        return jax.random.normal(subkeys[key_idx], arr_shape, jnp.float32) * std_dev

    cache_shape = (LAYERS, BATCH, SMAX, HEADS, HEAD)
    positions = jax.random.randint(subkeys[1], (BATCH,), 0, SMAX, dtype=jnp.int32)
    positions = positions.at[0].set(SMAX - 1)
    v_mean = normal(3, (LAYERS, BATCH, 1, HEADS, HEAD), 1.0)
    return {
        'x_embed': normal(0, (BATCH, D), 1.0).astype(jnp.bfloat16),
        'positions': positions,
        'k_cache': normal(2, cache_shape, 1.0).astype(jnp.bfloat16),
        'v_cache': (v_mean + normal(4, cache_shape, 0.5)).astype(jnp.bfloat16),
        'ln1_gain': (1.0 + normal(5, (LAYERS, D), 0.2)).astype(jnp.bfloat16),
        'ln1_bias': normal(6, (LAYERS, D), 0.2).astype(jnp.bfloat16),
        'ln2_gain': (1.0 + normal(7, (LAYERS, D), 0.2)).astype(jnp.bfloat16),
        'ln2_bias': normal(8, (LAYERS, D), 0.2).astype(jnp.bfloat16),
        'w_qkv': normal(9, (LAYERS, D, 3 * D), D ** -0.5).astype(jnp.bfloat16),
        'b_qkv': normal(10, (LAYERS, 3 * D), 0.3).astype(jnp.bfloat16),
        'w_out': normal(11, (LAYERS, D, D), D ** -0.5).astype(jnp.bfloat16),
        'b_out': normal(12, (LAYERS, D), 0.3).astype(jnp.bfloat16),
        'w_in': normal(13, (LAYERS, D, FF), D ** -0.5).astype(jnp.bfloat16),
        'b_in': normal(14, (LAYERS, FF), 0.3).astype(jnp.bfloat16),
        'w_down': normal(15, (LAYERS, FF, D), FF ** -0.5).astype(jnp.bfloat16),
        'b_down': normal(16, (LAYERS, D), 0.3).astype(jnp.bfloat16),
        'lnf_gain': (1.0 + normal(17, (D,), 0.2)).astype(jnp.bfloat16),
        'lnf_bias': normal(18, (D,), 0.2).astype(jnp.bfloat16),
    }


def layer_norm(values, ln_gain, ln_bias):
    x_f32 = values.astype(jnp.float32)
    row_mean = jnp.mean(x_f32, axis=-1, keepdims=True)
    centered = x_f32 - row_mean
    row_var = jnp.mean(centered * centered, axis=-1, keepdims=True)
    normed = centered * lax.rsqrt(row_var + LN_EPS)
    return (normed * ln_gain.astype(jnp.float32) + ln_bias.astype(jnp.float32)).astype(jnp.bfloat16)


def rotate(values, cos_t, sin_t):
    half_dim = ROT // 2
    rot_part = values[..., :ROT].astype(jnp.float32)
    turned = jnp.concatenate([-rot_part[..., half_dim:], rot_part[..., :half_dim]], axis=-1)
    mixed = rot_part * cos_t + turned * sin_t
    return jnp.concatenate([mixed.astype(jnp.bfloat16), values[..., ROT:]], axis=-1)


def reference(x_embed, positions, k_cache, v_cache, ln1_gain, ln1_bias, ln2_gain, ln2_bias, w_qkv, b_qkv, w_out, b_out, w_in, b_in, w_down, b_down, lnf_gain, lnf_bias):
    inv_freq = 1.0 / (ROPE_BASE ** (jnp.arange(0, ROT, 2).astype(jnp.float32) / ROT))
    angles = positions.astype(jnp.float32)[:, None] * inv_freq[None, :]
    angles = jnp.concatenate([angles, angles], axis=-1)[:, None, :]
    cos_t = jnp.cos(angles)
    sin_t = jnp.sin(angles)
    slot_ids = jnp.arange(SMAX)
    write_mask = (slot_ids[None, :] == positions[:, None])[:, :, None, None]
    keep_mask = (slot_ids[None, :] <= positions[:, None])[:, None, :]

    def one_layer(hidden, params):
        (k_layer, v_layer, g_one, c_one, g_two, c_two, wqkv_l, bqkv_l, wout_l, bout_l, win_l, bin_l, wdown_l, bdown_l) = params
        h_attn = layer_norm(hidden, g_one, c_one)
        h_mlp = layer_norm(hidden, g_two, c_two)
        qkv_proj = (jnp.dot(h_attn, wqkv_l, preferred_element_type=jnp.float32) + bqkv_l.astype(jnp.float32)).astype(jnp.bfloat16)
        qkv_proj = qkv_proj.reshape(BATCH, HEADS, 3, HEAD)
        q_heads = rotate(qkv_proj[:, :, 0], cos_t, sin_t)
        k_heads = rotate(qkv_proj[:, :, 1], cos_t, sin_t)
        v_heads = qkv_proj[:, :, 2]
        k_layer = jnp.where(write_mask, k_heads[:, None], k_layer)
        v_layer = jnp.where(write_mask, v_heads[:, None], v_layer)
        scores = jnp.einsum('bhd,bshd->bhs', q_heads.astype(jnp.float32), k_layer.astype(jnp.float32)) * (HEAD ** -0.5)
        scores = jnp.where(keep_mask, scores, -jnp.inf)
        attn_probs = jax.nn.softmax(scores, axis=-1).astype(jnp.bfloat16)
        context = jnp.einsum('bhs,bshd->bhd', attn_probs.astype(jnp.float32), v_layer.astype(jnp.float32)).astype(jnp.bfloat16).reshape(BATCH, D)
        attn_out = jnp.dot(context, wout_l, preferred_element_type=jnp.float32) + bout_l.astype(jnp.float32)
        mlp_act = jax.nn.gelu(jnp.dot(h_mlp, win_l, preferred_element_type=jnp.float32) + bin_l.astype(jnp.float32), approximate=False).astype(jnp.bfloat16)
        mlp_out = jnp.dot(mlp_act, wdown_l, preferred_element_type=jnp.float32) + bdown_l.astype(jnp.float32)
        hidden = (hidden.astype(jnp.float32) + attn_out + mlp_out).astype(jnp.bfloat16)
        return hidden, (k_layer, v_layer)

    stacked = (k_cache, v_cache, ln1_gain, ln1_bias, ln2_gain, ln2_bias, w_qkv, b_qkv, w_out, b_out, w_in, b_in, w_down, b_down)
    hidden, (k_new, v_new) = lax.scan(one_layer, x_embed, stacked)
    return layer_norm(hidden, lnf_gain, lnf_bias), k_new, v_new
```

```python
import functools
import jax
import jax.numpy as jnp
from jax import lax
from jax.experimental import pallas as pl
from jax.experimental.pallas import tpu as pltpu
from jax.sharding import PartitionSpec as P

LN_EPS = 1e-5
ROPE_BASE = 10000.0
MESH = pl.DeviceIdType.MESH
NZ = 4
Z, Y, X, C = 0, 1, 2, 3
VEC_ROWS = 24


def layer_norm(values, ln_gain, ln_bias):
    x_f32 = values.astype(jnp.float32)
    row_mean = jnp.mean(x_f32, axis=-1, keepdims=True)
    centered = x_f32 - row_mean
    row_var = jnp.mean(centered * centered, axis=-1, keepdims=True)
    normed = centered * lax.rsqrt(row_var + LN_EPS)
    return (normed * ln_gain.astype(jnp.float32) + ln_bias.astype(jnp.float32)).astype(jnp.bfloat16)


def rope_tables(positions, rot_dim):
    inv_freq = 1.0 / (ROPE_BASE ** (jnp.arange(0, rot_dim, 2).astype(jnp.float32) / rot_dim))
    angles = positions.astype(jnp.float32)[:, None] * inv_freq[None, :]
    angles = jnp.concatenate([angles, angles], axis=-1)[:, None, :]
    return jnp.cos(angles), jnp.sin(angles)


def rotate(values, cos_t, sin_t):
    rot_dim = cos_t.shape[-1]
    half_dim = rot_dim // 2
    rot_part = values[..., :rot_dim].astype(jnp.float32)
    turned = jnp.concatenate([-rot_part[..., half_dim:], rot_part[..., :half_dim]], axis=-1)
    mixed = rot_part * cos_t + turned * sin_t
    return jnp.concatenate([mixed.astype(jnp.bfloat16), values[..., rot_dim:]], axis=-1)


def attention(q_heads, k_heads, v_heads, k_cache, v_cache, positions):
    slot_ids = jnp.arange(k_cache.shape[1], dtype=jnp.int32)
    write_mask = (slot_ids[None, :] == positions[:, None])[:, :, None, None]
    k_cache = jnp.where(write_mask, k_heads[:, None], k_cache)
    v_cache = jnp.where(write_mask, v_heads[:, None], v_cache)
    scores = jnp.einsum('bhd,bshd->bhs', q_heads, k_cache, preferred_element_type=jnp.float32) * (q_heads.shape[-1] ** -0.5)
    keep_mask = (slot_ids[None, :] <= positions[:, None])[:, None, :]
    scores = jnp.where(keep_mask, scores, -jnp.inf)
    attn_probs = jax.nn.softmax(scores, axis=-1).astype(jnp.bfloat16)
    context = jnp.einsum('bhs,bshd->bhd', attn_probs, v_cache, preferred_element_type=jnp.float32).astype(jnp.bfloat16)
    return context.reshape(context.shape[0], -1), k_cache, v_cache


def decode_layer(hidden, positions, cos_t, sin_t, k_cache, v_cache, params):
    ln1_gain, ln1_bias, ln2_gain, ln2_bias, w_qkv, b_qkv, w_out, b_out, w_in, b_in, w_down, b_down = params
    n_heads, head_dim = k_cache.shape[2], k_cache.shape[3]
    h_attn = layer_norm(hidden, ln1_gain, ln1_bias)
    h_mlp = layer_norm(hidden, ln2_gain, ln2_bias)
    qkv_proj = (jnp.dot(h_attn, w_qkv, preferred_element_type=jnp.float32) + b_qkv.astype(jnp.float32)).astype(jnp.bfloat16)
    qkv_proj = qkv_proj.reshape(hidden.shape[0], n_heads, 3, head_dim)
    q_heads = rotate(qkv_proj[:, :, 0], cos_t, sin_t)
    k_heads = rotate(qkv_proj[:, :, 1], cos_t, sin_t)
    context, k_cache, v_cache = attention(q_heads, k_heads, qkv_proj[:, :, 2], k_cache, v_cache, positions)
    attn_out = jnp.dot(context, w_out, preferred_element_type=jnp.float32) + b_out.astype(jnp.float32)
    mlp_act = jax.nn.gelu(jnp.dot(h_mlp, w_in, preferred_element_type=jnp.float32) + b_in.astype(jnp.float32), approximate=False).astype(jnp.bfloat16)
    mlp_out = jnp.dot(mlp_act, w_down, preferred_element_type=jnp.float32) + b_down.astype(jnp.float32)
    hidden = (hidden.astype(jnp.float32) + attn_out + mlp_out).astype(jnp.bfloat16)
    return hidden, k_cache, v_cache


ORDERS = ((Z, X, Y), (Z, Y, X), (X, Y, Z), (Y, X, Z))
SPLITS = {'qkv': (7, 7, 2, 2), 'win': (10, 10, 2, 2), 'out': (3, 3, 0, 0), 'down': (2, 2, 1, 1)}
SEMS = 9


class Part:
    def __init__(self, ref, own_ref, layer, cols, order, where, sems):
        self.ref, self.own_ref, self.layer, self.cols, self.order, self.where = ref, own_ref, layer, cols, order, where
        self.send_sems, self.recv_sems, self.index = sems

    def block(self, full, where):
        sel = tuple(pl.ds(0, (4, 2, 2)[d]) if d in full else where[d] for d in (Z, Y, X))
        if C in full:
            raise ValueError
        return self.ref.at[(self.layer,) + sel + (where[C], slice(None), self.cols)]

    def copy(self, full, where, slot, device):
        blk = self.block(full, where)
        return pltpu.make_async_remote_copy(
            src_ref=blk, dst_ref=blk, send_sem=self.send_sems.at[self.index, slot], recv_sem=self.recv_sems.at[self.index, slot],
            device_id=(device,), device_id_type=MESH)

    def dev(self, **moved):
        w = dict(z=self.where[Z], y=self.where[Y], x=self.where[X], c=self.where[C])
        w.update(moved)
        return ((w['z'] * 2 + w['y']) * 2 + w['x']) * 2 + w['c']

    def moved(self, d, value):
        w = list(self.where)
        w[d] = value
        return tuple(w)

    def _xy(self, d, full):
        other = 1 - self.where[d]
        return self.copy(full, self.where, 6 if d == X else 7, self.dev(x=other) if d == X else self.dev(y=other))

    def _up(self, full, hop):
        z = self.where[Z]
        return self.copy(full, self.moved(Z, z - hop), hop, self.dev(z=z + 1))

    def _down(self, full, hop):
        z = self.where[Z]
        return self.copy(full, self.moved(Z, z + hop), 3 + hop, self.dev(z=z - 1))

    def start(self, phase):
        d, full = self.order[phase], self.order[:phase]
        if d != Z:
            self._xy(d, full).start()
            return
        z = self.where[Z]

        @pl.when(z < NZ - 1)
        def _():
            self._up(full, 0).start()

        @pl.when(z > 0)
        def _():
            self._down(full, 0).start()

    def finish(self, phase):
        d, full = self.order[phase], self.order[:phase]
        if d != Z:
            self._xy(d, full).wait_recv()
            return
        z = self.where[Z]
        for hop in range(NZ - 1):
            @pl.when(z - hop - 1 >= 0)
            def _():
                self._up(full, hop).wait_recv()
                if hop < NZ - 2:
                    @pl.when(z < NZ - 1)
                    def _():
                        self._up(full, hop + 1).start()

            @pl.when(z + hop + 1 < NZ)
            def _():
                self._down(full, hop).wait_recv()
                if hop < NZ - 2:
                    @pl.when(z > 0)
                    def _():
                        self._down(full, hop + 1).start()

    def partner(self):
        return self.copy((Z, Y, X), self.where, 8, self.dev(c=1 - self.where[C]))

    def drain(self):
        for phase in range(3):
            d, full = self.order[phase], self.order[:phase]
            if d != Z:
                self._xy(d, full).wait_send()
                continue
            z = self.where[Z]
            for hop in range(NZ - 1):
                @pl.when((z < NZ - 1) & (z - hop >= 0))
                def _():
                    self._up(full, hop).wait_send()

                @pl.when((z > 0) & (z + hop < NZ))
                def _():
                    self._down(full, hop).wait_send()
        self.partner().wait_send()


def split_cols(family, count):
    out, at = [], 0
    for order, units in zip(ORDERS, SPLITS[family]):
        if units:
            out.append((order, pl.ds(at * 128, units * 128)))
            at += units
    assert at * 128 == count
    return out


def gather_kernel(shapes, vec_in, qkv_in, win_in, out_in, down_in, vec_g, qkv_g, win_g, out_g, down_g, own_sem, send_sems, recv_sems):
    me = lax.axis_index('dp')
    where = (me // 8, (me // 4) % 2, (me // 2) % 2, me % 2)
    z, y, x, c = where

    def at(z, y, x, c):
        return (((z * 2 + y) * 2 + x) * 2 + c,)

    pairs = ((vec_in, vec_g), (qkv_in, qkv_g), (win_in, win_g), (out_in, out_g), (down_in, down_g))
    own = []
    for i, (src, dst) in enumerate(pairs):
        cp = pltpu.make_async_copy(src, dst.at[:, z, y, x, c], own_sem.at[i])
        cp.start()
        own.append(cp)

    barrier = pltpu.get_barrier_semaphore()
    for who in (at(z, y, x, 1 - c), at(z, y, 1 - x, c), at(z, 1 - y, x, c)):
        pl.semaphore_signal(barrier, inc=1, device_id=who, device_id_type=MESH)

    @pl.when(z > 0)
    def _():
        pl.semaphore_signal(barrier, inc=1, device_id=at(z - 1, y, x, c), device_id_type=MESH)

    @pl.when(z < NZ - 1)
    def _():
        pl.semaphore_signal(barrier, inc=1, device_id=at(z + 1, y, x, c), device_id_type=MESH)

    pl.semaphore_wait(barrier, 3 + (z + 3) // 4 + (6 - z) // 4)

    for cp in own:
        cp.wait()

    groups, index = [], 0
    sems = lambda i: (send_sems, recv_sems, i)
    groups.append([Part(vec_g, vec_in, 0, pl.ds(0, 128), ORDERS[0], where, sems(0))])
    index = 1
    for layer in range(2):
        for family, ref, src in (('qkv', qkv_g, qkv_in), ('win', win_g, win_in), ('out', out_g, out_in), ('down', down_g, down_in)):
            group = []
            for order, cols in split_cols(family, shapes[family]):
                group.append(Part(ref, src, layer, cols, order, where, sems(index)))
                index += 1
            groups.append(group)

    n = len(groups)
    for t in range(n + 4):
        def each(k):
            return groups[k] if 0 <= k < n else []
        if t == 0:
            for p in each(0):
                p.start(0)
        for p in each(t + 1):
            p.start(0)
        for p in each(t - 3):
            p.partner().wait_recv()
        for phase in (2, 1, 0):
            for p in each(t - phase):
                p.finish(phase)
                if phase < 2:
                    p.start(phase + 1)
                else:
                    p.partner().start()
    for group in groups:
        for p in group:
            p.drain()


def gather_all(vec, w_qkv, w_in, w_out, w_down):
    f = lambda a: jax.ShapeDtypeStruct((a.shape[0], 4, 2, 2, 2) + a.shape[1:], a.dtype)
    ins = (vec, w_qkv, w_in, w_out, w_down)
    shapes = {'qkv': w_qkv.shape[2], 'win': w_in.shape[2], 'out': w_out.shape[2], 'down': w_down.shape[2]}
    parts = 1 + 2 * sum(sum(1 for u in s if u) for s in SPLITS.values())
    return pl.pallas_call(
        functools.partial(gather_kernel, shapes),
        out_shape=tuple(f(a) for a in ins),
        in_specs=[pl.BlockSpec(memory_space=pl.ANY)] * 5,
        out_specs=[pl.BlockSpec(memory_space=pltpu.VMEM)] * 5,
        scratch_shapes=[pltpu.SemaphoreType.DMA((5,)), pltpu.SemaphoreType.DMA((parts, SEMS)), pltpu.SemaphoreType.DMA((parts, SEMS))],
        compiler_params=pltpu.CompilerParams(collective_id=0, has_side_effects=True, vmem_limit_bytes=60000 * 1024),
    )(*ins)


def solution(mesh):
    row_spec = P('dp', None)
    vec_spec = P(None, 'dp')
    mat_spec = P(None, 'dp', None)
    cache_spec = P(None, 'dp', None, None, None)
    in_specs = (row_spec, P('dp'), cache_spec, cache_spec, vec_spec, vec_spec, vec_spec, vec_spec, mat_spec, vec_spec, mat_spec, vec_spec, mat_spec, vec_spec, mat_spec, vec_spec, P('dp'), P('dp'))
    out_specs = (row_spec, cache_spec, cache_spec)

    def device_step(x_embed, positions, k_cache, v_cache, ln1_gain, ln1_bias, ln2_gain, ln2_bias, w_qkv, b_qkv, w_out, b_out, w_in, b_in, w_down, b_down, lnf_gain, lnf_bias):
        vecs = (ln1_gain, ln1_bias, ln2_gain, ln2_bias, b_out, b_down, lnf_gain[None], lnf_bias[None], b_qkv, b_in)
        rows = jnp.concatenate([jnp.pad(v, ((0, 0), (0, 128 - v.shape[1]))) for v in vecs])
        vec = jnp.pad(rows, ((0, VEC_ROWS - rows.shape[0]), (0, 0))).astype(jnp.float32)[None]
        vec_g, qkv_g, win_g, out_g, down_g = gather_all(vec, w_qkv, w_in, w_out, w_down)
        vec_g = vec_g.reshape(32, VEC_ROWS, 128)
        row = [0]

        def take(v):
            got = [vec_g[:, row[0] + i, :v.shape[1]].reshape(-1) for i in range(v.shape[0])]
            row[0] += v.shape[0]
            return got

        g1, c1, g2, c2, bo, bd, gf, cf, bq, bi = [take(v) for v in vecs]
        mats = [a.reshape(2, -1, a.shape[-1]) for a in (qkv_g, out_g, win_g, down_g)]
        cos_t, sin_t = rope_tables(positions, k_cache.shape[4] // 4)
        hidden = x_embed
        k_list = []
        v_list = []
        for i in range(2):
            params = (g1[i], c1[i], g2[i], c2[i], mats[0][i], bq[i], mats[1][i], bo[i], mats[2][i], bi[i], mats[3][i], bd[i])
            hidden, k_new, v_new = decode_layer(hidden, positions, cos_t, sin_t, k_cache[i], v_cache[i], params)
            k_list.append(k_new)
            v_list.append(v_new)
        return layer_norm(hidden, gf[0], cf[0]), jnp.stack(k_list), jnp.stack(v_list)

    return jax.shard_map(device_step, mesh=mesh, in_specs=in_specs, out_specs=out_specs, check_vma=False)
```

```python
import functools
import jax
import jax.numpy as jnp
from jax import lax
from jax.experimental import pallas as pl
from jax.experimental.pallas import tpu as pltpu
from jax.sharding import PartitionSpec as P

LN_EPS = 1e-5
ROPE_BASE = 10000.0
MESH = pl.DeviceIdType.MESH
F32, BF16 = jnp.float32, jnp.bfloat16
NZ = 4
Z, Y, X, C = 0, 1, 2, 3
DIMS = (4, 2, 2, 2)
VEC_ROWS = 24
ROWS, D, HEADS, HEAD, SLOTS, FF = 64, 768, 12, 64, 32, 3072
KEYS = HEADS * SLOTS
HID = FF // 2
SEQS = 8
BLOCKS = ROWS // SEQS
RING = 4
SENDS = 6


class Part:
    def __init__(self, ref, lead, cols, order, where, sems, held=(Z, Y, X), first=None):
        self.ref, self.lead, self.cols, self.order, self.where = ref, lead, cols, order, where
        self.send_sems, self.recv_sems, self.index = sems
        self.held, self.first = held, first

    def block(self, full, where):
        sel = tuple(pl.ds(0, DIMS[d]) if d in full else where[d] for d in self.held)
        return self.ref.at[self.lead + sel + (where[C], slice(None), self.cols)]

    def device(self, d, value):
        w = list(self.where)
        w[d] = value
        return (((w[0] * 2 + w[1]) * 2 + w[2]) * 2 + w[3],)

    def copies(self, phase):
        d = self.order[phase] if phase < len(self.order) else C
        full = self.order[:phase]
        if self.order[0] == Y and phase > 0 and self.first is not None:
            full = (Y,) + tuple(self.order[1:phase])
        if d == Z:
            targets = [(k, (self.where[Z] + k + 1) % NZ) for k in range(NZ - 1)]
        else:
            targets = [({X: 3, Y: 4, C: 5}[d], 1 - self.where[d])]
        blk = self.block(full, self.where)
        src = self.first if (phase == 0 and self.first is not None) else blk
        return [pltpu.make_async_remote_copy(
            src_ref=src, dst_ref=blk, send_sem=self.send_sems.at[self.index, k], recv_sem=self.recv_sems.at[self.index, k],
            device_id=self.device(d, to), device_id_type=MESH) for k, to in targets]

    @property
    def phases(self):
        return len(self.order) + 1

    def start(self, phase):
        for cp in self.copies(phase):
            cp.start()

    def finish(self, phase):
        for cp in self.copies(phase):
            cp.wait_recv()

    def drain(self):
        for phase in range(self.phases):
            for cp in self.copies(phase):
                cp.wait_send()


def iota(shape, axis):
    return lax.broadcasted_iota(jnp.int32, shape, axis)


def floor_div(values, width):
    return jnp.floor((values + 0.5) * (1.0 / width))


def dot(a, b):
    return jnp.dot(a, b, preferred_element_type=F32)


def layer_norm(x_f32, gain, bias):
    row_mean = jnp.mean(x_f32, axis=-1, keepdims=True)
    centered = x_f32 - row_mean
    row_var = jnp.mean(centered * centered, axis=-1, keepdims=True)
    return (centered * lax.rsqrt(row_var + LN_EPS) * gain + bias).astype(BF16)


def one_hot_cols(width, cols_f32):
    index = cols_f32 - floor_div(cols_f32, width) * width
    return (iota(index.shape, 0).astype(F32) == index).astype(BF16)


def kernel(pos_ref, x_ref, rope_ref, vec_ref, qkv_ref, out_ref, win_ref, down_ref, k_hbm, v_hbm,
           y_ref, ko_hbm, vo_hbm,
           vec_g, qkv_g, out_g, win_g, down_g, x1_scr, xn_scr, ps_scr, pr_scr, h1_scr, h2_scr, act_scr, acc_scr,
           vrow_scr, bq_scr, bi_scr, q_scr, kn_scr, vn_scr, ctx_scr, s_scr, kbuf, vbuf,
           own_sem, send_sems, recv_sems, xs_sem, xr_sem, ps_sem, pr_sem, in_sem, out_sem):
    me = lax.axis_index('dp')
    where = (me // 8, (me // 4) % 2, (me // 2) % 2, me % 2)
    z, y, x, c = where

    def device(z, y, x, c):
        return (((z * 2 + y) * 2 + x) * 2 + c,)

    y_peer = device(z, 1 - y, x, c)

    def cache_in(i):
        l, blk, slot = i // BLOCKS, i % BLOCKS, i % RING
        rows = pl.ds(blk * SEQS, SEQS)
        return [pltpu.make_async_copy(k_hbm.at[l, rows], kbuf.at[slot], in_sem.at[0, slot]),
                pltpu.make_async_copy(v_hbm.at[l, rows], vbuf.at[slot], in_sem.at[1, slot])]

    def cache_out(i):
        l, blk, slot = i // BLOCKS, i % BLOCKS, i % RING
        rows = pl.ds(blk * SEQS, SEQS)
        return [pltpu.make_async_copy(kbuf.at[slot], ko_hbm.at[l, rows], out_sem.at[0, slot]),
                pltpu.make_async_copy(vbuf.at[slot], vo_hbm.at[l, rows], out_sem.at[1, slot])]

    def my_cols(zb, yy):
        return pl.ds(pl.multiple_of(768 * zb + 384 * yy, 128), 384)

    own = [(vec_ref, vec_g.at[0, z, y, x, c]), (qkv_ref.at[0], qkv_g.at[0, z, y, x, c])]
    own += [(win_ref.at[0, :, my_cols(zb, y)], win_g.at[0, z, y, x, c, :, pl.ds(384 * zb, 384)]) for zb in range(4)]
    own += [(down_ref.at[0], down_g.at[0, z, x, c]), (out_ref.at[0], out_g.at[0, z, y, x, c]), (qkv_ref.at[1], qkv_g.at[1, z, y, x, c])]
    own += [(win_ref.at[1, :, my_cols(zb, y)], win_g.at[1, z, y, x, c, :, pl.ds(384 * zb, 384)]) for zb in range(4)]
    own += [(down_ref.at[1], down_g.at[1, z, x, c]), (out_ref.at[1], out_g.at[1, z, y, x, c])]
    own = [pltpu.make_async_copy(src, dst, own_sem.at[i]) for i, (src, dst) in enumerate(own)]
    for cp in own:
        cp.start()

    barrier = pltpu.get_barrier_semaphore()
    peers = [device((z + k) % NZ, y, x, c) for k in range(1, NZ)] + [device(z, y, 1 - x, c), y_peer, device(z, y, x, 1 - c)]
    for who in peers:
        pl.semaphore_signal(barrier, inc=1, device_id=who, device_id_type=MESH)
    pl.semaphore_wait(barrier, len(peers))
    for cp in own:
        cp.wait()
    for i in range(RING - 1):
        for cp in cache_in(i):
            cp.start()

    sems = lambda i: (send_sems, recv_sems, i)
    counter = [0]

    def part(*args, **kw):
        counter[0] += 1
        return Part(*args, where, sems(counter[0] - 1), **kw)

    def qkv_group(l, i):
        return [part(qkv_g, (l,), pl.ds(768 * i, 384), (Z, X, Y)), part(qkv_g, (l,), pl.ds(768 * i + 384, 384), (Z, Y, X))]

    def win_group(l, zb):
        first = win_ref.at[l, :, my_cols(zb, 1 - y)]
        return [part(win_g, (l,), pl.ds(384 * zb, 384), (Y, Z, X), first=first)]

    def down_group(l, i):
        return [part(down_g, (l,), pl.ds(384 * i, 384), (Z, X), held=(Z, X))]

    def out_group(l):
        return [part(out_g, (l,), pl.ds(0, 768), (Z, X, Y))]

    names, groups = [], []

    def add(name, parts):
        names.append(name)
        groups.append(parts)

    add('vec', [part(vec_g, (0,), pl.ds(0, 128), (Z, X, Y))])
    for l in range(2):
        for i in range(3):
            add(f'qkv{l}{i}', qkv_group(l, i))
        for i in range(4):
            add(f'win{l}{i}', win_group(l, i))
        for i in range(2):
            add(f'down{l}{i}', down_group(l, i))
        add(f'out{l}', out_group(l))

    lane = iota((1, 128), 1)

    def send_x(l):
        src = x_ref if l == 0 else x1_scr
        return pltpu.make_async_remote_copy(src_ref=src, dst_ref=xn_scr.at[l], send_sem=xs_sem.at[l], recv_sem=xr_sem.at[l],
                                            device_id=y_peer, device_id_type=MESH)

    def send_part(l):
        return pltpu.make_async_remote_copy(src_ref=ps_scr.at[l], dst_ref=pr_scr.at[l], send_sem=ps_sem.at[l], recv_sem=pr_sem.at[l],
                                            device_id=y_peer, device_id_type=MESH)

    def task_vec():
        vec2 = vec_g[...].reshape(32 * VEC_ROWS, 128).astype(BF16)
        n = iota((1, D), 1).astype(F32)
        spread = dot(vec2, one_hot_cols(24, jnp.broadcast_to(n, (128, D))))
        r = iota((32 * VEC_ROWS, 1), 0).astype(F32)
        mine = floor_div(n, 24) == floor_div(r, VEC_ROWS)
        spread = jnp.where(mine, spread, 0.0).astype(BF16)
        rr = iota((1, 32 * VEC_ROWS), 1).astype(F32)
        kind = rr - floor_div(rr, VEC_ROWS) * VEC_ROWS
        pick = (iota((VEC_ROWS, 32 * VEC_ROWS), 0).astype(F32) == kind).astype(BF16)
        vrow_scr[...] = dot(pick, spread)
        dev = iota((32, 1), 0).astype(F32)

        def long_row(kind, width, cols):
            g = vec_g[0, :, :, :, :, kind].reshape(32, 128).astype(BF16)
            n = cols.astype(F32)
            full = dot(g, one_hot_cols(width, jnp.broadcast_to(n, (128, n.shape[1]))))
            return jnp.sum(jnp.where(floor_div(n, width) == dev, full, 0.0), axis=0, keepdims=True)

        for l in range(2):
            bq_scr[l] = long_row(14 + l, 72, iota((1, 3 * D), 1))
            for zb in range(4):
                bi_scr[l, :, pl.ds(384 * zb, 384)] = long_row(16 + l, 96, iota((1, 384), 1) + (768 * zb + 384 * y))

    def vrow(kind):
        return vrow_scr[pl.ds(kind, 1), :]

    def x_of(l):
        return (x_ref if l == 0 else x1_scr)[...]

    def task_start(l):
        send_x(l).start()
        h1_scr[...] = layer_norm(x_of(l).astype(F32), vrow(l), vrow(2 + l))

    def task_qkv(l, i):
        w = qkv_g[l, :, :, :, :, :, pl.ds(768 * i, 768)].reshape(D, 768)
        got = (dot(h1_scr[...], w) + bq_scr[l, :, pl.ds(768 * i, 768)]).astype(BF16).astype(F32)
        for m in range(2):
            tiles = []
            for t in range(3):
                v = got[:, 384 * m + 128 * t: 384 * m + 128 * t + 128]
                r = v * rope_ref[3 * t] + pltpu.roll(v, 120, 1) * rope_ref[3 * t + 1] + pltpu.roll(v, 8, 1) * rope_ref[3 * t + 2]
                tiles.append(r.astype(BF16).astype(F32))
            h = 4 * i + 2 * m
            t0, t1, t2 = tiles
            q_scr[pl.ds(h, ROWS, stride=16), :] = t0
            kn_scr[pl.ds(h, ROWS, stride=16), :] = pltpu.roll(t0, 64, 1)
            vn_scr[pl.ds(h, ROWS, stride=16), :] = t1
            q_scr[pl.ds(h + 1, ROWS, stride=16), :] = pltpu.roll(t1, 64, 1)
            kn_scr[pl.ds(h + 1, ROWS, stride=16), :] = t2
            vn_scr[pl.ds(h + 1, ROWS, stride=16), :] = pltpu.roll(t2, 64, 1)

    def task_att(l, blk):
        i = l * BLOCKS + blk
        slot = i % RING
        for cp in cache_in(i):
            cp.wait()
        key = iota((1, KEYS), 1)
        head_row = jnp.minimum(iota((16, 1), 0), HEADS - 1) * SLOTS
        slot_of = key - head_row
        own_head = (slot_of >= 0) & (slot_of < SLOTS)
        slots = iota((SLOTS, HEAD), 0)

        def scores(j):
            b = blk * SEQS + j
            pos = pos_ref[b]
            rows = pl.ds(b * 16, 16)
            put = jnp.where(slots == pos, 1.0, 0.0).astype(BF16) > 0.5

            def placed(buf, new_scr):
                new = new_scr[rows, :][:HEADS, :HEAD].astype(BF16)
                both = jnp.where(put[None], new[:, None, :], buf[slot, j])
                buf[slot, j] = both
                return both.reshape(KEYS, HEAD)

            keys = placed(kbuf, kn_scr)
            placed(vbuf, vn_scr)
            q = q_scr[rows, :][:, :HEAD].astype(BF16)
            s = lax.dot_general(q, keys, (((1,), (1,)), ((), ())), preferred_element_type=F32) * (HEAD ** -0.5)
            s_scr[pl.ds(j * 16, 16), :] = jnp.where(own_head & (slot_of <= pos), s, -jnp.inf)

        def weighted(j):
            p = s_scr[pl.ds(j * 16, 16), :].astype(BF16)
            got = dot(p, vbuf[slot, j].reshape(KEYS, HEAD))
            ctx_scr[pl.ds((blk * SEQS + j) * 16, 16), pl.ds(0, HEAD)] = got

        for j in range(SEQS):
            scores(j)
        s = s_scr[...]
        e = jnp.exp(s - jnp.max(s, axis=-1, keepdims=True))
        s_scr[...] = e / jnp.sum(e, axis=-1, keepdims=True)
        for j in range(SEQS):
            weighted(j)
        for cp in cache_out(i):
            cp.start()
        if i + RING - 1 < 2 * BLOCKS:
            if i >= 1:
                for cp in cache_out(i - 1):
                    cp.wait()
            for cp in cache_in(i + RING - 1):
                cp.start()

    def task_h2(l):
        send_x(l).wait_recv()
        for half, v in enumerate((x_of(l), xn_scr[l])):
            h2_scr[pl.ds(ROWS * half, ROWS), :] = layer_norm(v.astype(F32), vrow(4 + l), vrow(6 + l))

    def task_win(l, zb):
        cols = pl.ds(384 * zb, 384)
        w = win_g[l, :, :, :, :, :, cols].reshape(D, 384)
        u = dot(h2_scr[...], w) + bi_scr[l, :, cols]
        act_scr[:, cols] = (0.5 * u * (1.0 + lax.erf(u * 0.7071067811865476))).astype(BF16)

    def task_down(l, i):
        cols = pl.ds(384 * i, 384)
        got = dot(act_scr[...], down_g[l, :, :, :, :, cols].reshape(HID, 384))
        acc_scr[:, cols] = got[:ROWS]
        ps_scr[l, :, cols] = got[ROWS:]
        if i == 1:
            send_part(l).start()

    def task_out(l):
        tiles = []
        for m in range(HEADS // 2):
            a = ctx_scr[pl.ds(2 * m, ROWS, stride=16), :]
            b = pltpu.roll(ctx_scr[pl.ds(2 * m + 1, ROWS, stride=16), :], 64, 1)
            tiles.append(jnp.where(lane < 64, a, b).astype(BF16))
        a = dot(jnp.concatenate(tiles, axis=1), out_g[l].reshape(D, D)) + vrow(8 + l)
        send_part(l).wait_recv()
        m = acc_scr[...] + pr_scr[l] + vrow(10 + l)
        new = (x_of(l).astype(F32) + a + m).astype(BF16)
        if l == 0:
            x1_scr[...] = new
        else:
            y_ref[...] = layer_norm(new.astype(F32), vrow(12), vrow(13))

    tasks = []

    def task(name, fn, needs, after, cost):
        tasks.append((name, fn, set(needs), set(after), cost))

    task('vec', task_vec, ['vec'], [], 2.0)
    for l in range(2):
        task(f's{l}', functools.partial(task_start, l), [], ['vec'] if l == 0 else ['o0'], 0.4)
        for i in range(3):
            task(f'q{l}{i}', functools.partial(task_qkv, l, i), [f'qkv{l}{i}'], [f's{l}'], 0.8)
        task(f'h{l}', functools.partial(task_h2, l), [], [f's{l}', f'q{l}2'], 0.6)
        for i in range(4):
            task(f'w{l}{i}', functools.partial(task_win, l, i), [f'win{l}{i}'], [f'h{l}'], 0.8)
        for i in range(2):
            task(f'd{l}{i}', functools.partial(task_down, l, i), [f'down{l}{i}'], [f'w{l}{k}' for k in range(4)], 0.8)
        for i in range(BLOCKS):
            task(f'a{l}{i}', functools.partial(task_att, l, i), [], [f'q{l}{k}' for k in range(3)], 1.4)
        task(f'o{l}', functools.partial(task_out, l), [f'out{l}'], [f'a{l}{k}' for k in range(BLOCKS)] + [f'd{l}0', f'd{l}1'], 0.8)

    done_groups, done_tasks = set(), set()

    def run(budget):
        while budget > 0:
            for entry in tasks:
                name, fn, needs, after, cost = entry
                if name not in done_tasks and needs <= done_groups and after <= done_tasks:
                    fn()
                    done_tasks.add(name)
                    budget -= cost
                    break
            else:
                return

    n = len(groups)
    for p in groups[0]:
        p.start(0)
    for t in range(n + 5):
        if t + 1 < n:
            for p in groups[t + 1]:
                p.start(0)
        for age in (4, 3, 2, 1, 0):
            g = t - age
            if not 0 <= g < n:
                continue
            for p in groups[g]:
                if age < p.phases:
                    p.finish(age)
                    if age + 1 < p.phases:
                        p.start(age + 1)
                    else:
                        done_groups.add(names[g])
        run(2.2)
    run(1e9)
    assert len(done_tasks) == len(tasks)

    for group in groups:
        for p in group:
            p.drain()
    for l in range(2):
        send_x(l).wait_send()
        send_part(l).wait_send()
    for i in range(2 * BLOCKS - RING, 2 * BLOCKS):
        for cp in cache_out(i):
            cp.wait()


def fused(pos, x, rope, vec, w_qkv, w_out, w_in, w_down, k_cache, v_cache):
    parts = 1 + 2 * (6 + 4 + 2 + 1)
    vmem = pl.BlockSpec(memory_space=pltpu.VMEM)
    hbm = pl.BlockSpec(memory_space=pl.ANY)
    lead = (4, 2, 2, 2)
    dma = pltpu.SemaphoreType.DMA
    return pl.pallas_call(
        kernel,
        out_shape=(jax.ShapeDtypeStruct(x.shape, x.dtype), jax.ShapeDtypeStruct(k_cache.shape, k_cache.dtype), jax.ShapeDtypeStruct(v_cache.shape, v_cache.dtype)),
        in_specs=[pl.BlockSpec(memory_space=pltpu.SMEM), vmem, vmem] + [hbm] * 7,
        out_specs=[vmem, hbm, hbm],
        scratch_shapes=[
            pltpu.VMEM((1,) + lead + (VEC_ROWS, 128), F32),
            pltpu.VMEM((2,) + lead + (24, 3 * D), BF16),
            pltpu.VMEM((2,) + lead + (24, D), BF16),
            pltpu.VMEM((2,) + lead + (24, HID), BF16),
            pltpu.VMEM((2, 4, 2, 2, 96, D), BF16),
            pltpu.VMEM((ROWS, D), BF16),
            pltpu.VMEM((2, ROWS, D), BF16),
            pltpu.VMEM((2, ROWS, D), F32),
            pltpu.VMEM((2, ROWS, D), F32),
            pltpu.VMEM((ROWS, D), BF16),
            pltpu.VMEM((2 * ROWS, D), BF16),
            pltpu.VMEM((2 * ROWS, HID), BF16),
            pltpu.VMEM((ROWS, D), F32),
            pltpu.VMEM((VEC_ROWS, D), F32),
            pltpu.VMEM((2, 1, 3 * D), F32),
            pltpu.VMEM((2, 1, HID), F32),
            pltpu.VMEM((16 * ROWS, 128), F32),
            pltpu.VMEM((16 * ROWS, 128), F32),
            pltpu.VMEM((16 * ROWS, 128), F32),
            pltpu.VMEM((16 * ROWS, 128), F32),
            pltpu.VMEM((16 * SEQS, KEYS), F32),
            pltpu.VMEM((RING, SEQS, HEADS, SLOTS, HEAD), BF16),
            pltpu.VMEM((RING, SEQS, HEADS, SLOTS, HEAD), BF16),
            dma((17,)), dma((parts, SENDS)), dma((parts, SENDS)), dma((2,)), dma((2,)), dma((2,)), dma((2,)), dma((2, RING)), dma((2, RING)),
        ],
        compiler_params=pltpu.CompilerParams(collective_id=0, has_side_effects=True, vmem_limit_bytes=60000 * 1024),
    )(pos, x, rope, vec, w_qkv, w_out, w_in, w_down, k_cache, v_cache)


def rope_tables(positions):
    lane = jnp.arange(128)
    d = lane % HEAD
    freq = 1.0 / (ROPE_BASE ** ((2 * (d % 8)).astype(F32) / 16))
    angle = positions.astype(F32)[:, None] * freq[None, :]
    cos, sin = jnp.cos(angle), jnp.sin(angle)
    out = []
    for turned in (lane >= 0, lane >= 64, lane < 64):
        out += [jnp.where(turned & (d < 16), cos, 1.0), jnp.where(turned & (d < 8), -sin, 0.0), jnp.where(turned & (d >= 8) & (d < 16), sin, 0.0)]
    return jnp.stack(out)


def solution(mesh):
    row_spec = P('dp', None)
    vec_spec = P(None, 'dp')
    mat_spec = P(None, 'dp', None)
    cache_spec = P(None, 'dp', None, None, None)
    in_specs = (row_spec, P('dp'), cache_spec, cache_spec, vec_spec, vec_spec, vec_spec, vec_spec, mat_spec, vec_spec, mat_spec, vec_spec, mat_spec, vec_spec, mat_spec, vec_spec, P('dp'), P('dp'))
    out_specs = (row_spec, cache_spec, cache_spec)

    def device_step(x_embed, positions, k_cache, v_cache, ln1_gain, ln1_bias, ln2_gain, ln2_bias, w_qkv, b_qkv, w_out, b_out, w_in, b_in, w_down, b_down, lnf_gain, lnf_bias):
        vecs = (ln1_gain, ln1_bias, ln2_gain, ln2_bias, b_out, b_down, lnf_gain[None], lnf_bias[None], b_qkv, b_in)
        rows = jnp.concatenate([jnp.pad(v, ((0, 0), (0, 128 - v.shape[1]))) for v in vecs])
        vec = jnp.pad(rows, ((0, VEC_ROWS - rows.shape[0]), (0, 0))).astype(F32)
        by_head = lambda a: jnp.swapaxes(a, 2, 3)
        out, k_new, v_new = fused(positions, x_embed, rope_tables(positions), vec, w_qkv, w_out, w_in, w_down, by_head(k_cache), by_head(v_cache))
        return out, by_head(k_new), by_head(v_new)

    return jax.shard_map(device_step, mesh=mesh, in_specs=in_specs, out_specs=out_specs, check_vma=False)
```

```python
import collections
import functools
import heapq
import itertools
import math
import jax
import jax.numpy as jnp
import numpy as np
from jax import lax
from jax.experimental import pallas as pl
from jax.experimental.pallas import tpu as pltpu
from jax.sharding import PartitionSpec as P

LN_EPS = 1e-5
ROPE_BASE = 10000.0
MESH = pl.DeviceIdType.MESH
F32, BF16 = jnp.float32, jnp.bfloat16
NZ = 4
Z, Y, X, C = 0, 1, 2, 3
DIMS = (4, 2, 2, 2)
VEC_ROWS = 24
ROWS, D, HEADS, HEAD, SLOTS, FF = 64, 768, 12, 64, 32, 3072
KEYS = HEADS * SLOTS
HID = FF // 2
SEQS = 8
BLOCKS = ROWS // SEQS
VMEM_LIMIT, VMEM_SMALL = 36 << 20, 1 << 20
FREQS = tuple(float(np.float32(1.0) / np.float32(ROPE_BASE) ** (np.float32(2 * i) / np.float32(16))) for i in range(8))
FIRST = 7
SENDS = 6


LINK, CORES = 46600.0, 300000.0
FIXED, FIXED_CORES, HOP = 1.6, 0.9, 0.75
WINDOW, SLACK = 6, -0.5
SEQUENCE = (
    ('vec', 0, 0), ('qkv', 0, 0), ('qkv', 0, 1), ('qkv', 0, 2), ('win', 0, 0), ('win', 0, 1), ('win', 0, 2), ('win', 0, 3),
    ('qkv', 1, 0), ('down', 0, 0), ('qkv', 1, 1), ('down', 0, 1), ('out', 0, 0), ('qkv', 1, 2),
    ('win', 1, 0), ('win', 1, 1), ('win', 1, 2), ('win', 1, 3), ('down', 1, 0), ('down', 1, 1), ('out', 1, 0))


def group_parts(family, l, i):
    zxy, zyx = (Z, X, Y), (Z, Y, X)
    if family == 'vec':
        return [(family, l, 0, 128, zxy)]
    if family == 'qkv' and l == 1:
        return [(family, l, 768 * i, 768, zxy)]
    if family == 'win':
        return [(family, l, 384 * i, 384, (Y, Z, X))]
    if family == 'down':
        return [(family, l, 384 * i, 384, (Z, X))]
    return [(family, l, 768 * i, 384, zxy), (family, l, 768 * i + 384, 384, zyx)]


def sends(spec, phase, chip):
    family, _, _, width, order = spec
    size = width * {'vec': VEC_ROWS * 4, 'down': 192}.get(family, 48)
    for d in order[:phase]:
        size *= DIMS[d]
    if phase == len(order):
        return [(chip, size, [chip])]
    out, d = [], order[phase]
    for k in range(1, DIMS[d]):
        to = tuple((v + k) % DIMS[d] if e == d else v for e, v in enumerate(chip))
        up = to[d] > chip[d]
        path = range(chip[d], to[d]) if up else range(chip[d], to[d], -1)
        out.append((to, size, [(d, up) + tuple(v if e == d else w for e, w in enumerate(chip)) for v in path]))
    return out


def arrivals(groups):
    chips = list(itertools.product(range(4), range(2), range(2)))
    free, heap, got, times, set_out = {}, [], collections.Counter(), collections.defaultdict(list), {}

    def send(now, chip, g, i, phase):
        for to, size, links in sends(groups[g][i], phase, chip):
            own = to == chip
            begin = max([now] + [free.get(k, 0.0) for k in links])
            end = begin + size / (CORES if own else LINK)
            for k in links:
                free[k] = end
            heapq.heappush(heap, (end + (FIXED_CORES if own else FIXED + HOP * (len(links) - 1)), len(times), next(ticket), to, g, i, phase))

    ticket = itertools.count()
    for chip in chips:
        for g in range(WINDOW):
            for i in range(len(groups[g])):
                send(0.0, chip, g, i, 0)
        set_out[chip] = WINDOW
    while heap:
        now, _, _, chip, g, i, phase = heapq.heappop(heap)
        got[chip, g, i, phase] += 1
        spec = groups[g][i]
        if got[chip, g, i, phase] < len(sends(spec, phase, chip)):
            continue
        times[g, i, phase].append(now)
        if phase < len(spec[4]):
            send(now, chip, g, i, phase + 1)
        if phase == 0:
            got[chip, g] += 1
            if got[chip, g] == len(groups[g]) and set_out[chip] < len(groups):
                later = set_out[chip]
                set_out[chip] += 1
                for j in range(len(groups[later])):
                    send(now, chip, later, j, 0)
    return sorted((sum(v) / len(v), k) for k, v in times.items())


def compute_tasks():
    out = {'vec': ([('vec', 0, 0)], [], 2.0)}
    for l in range(2):
        out[f's{l}'] = ([], ['o0'] if l else ['vec'], 0.3)
        for i in range(3):
            out[f'q{l}{i}'] = ([('qkv', l, i)], [f's{l}'], 0.6)
        out[f'h{l}'] = ([], [f'q{l}2'], 0.5)
        for i in range(4):
            out[f'w{l}{i}'] = ([('win', l, i)], [f'h{l}'], 0.5)
        for i in range(2):
            out[f'd{l}{i}'] = ([('down', l, i)], [f'w{l}{k}' for k in range(4)], 0.5)
        for i in range(BLOCKS):
            out[f'a{l}{i}'] = ([], [f'q{l}{k}' for k in range(3)], 1.2)
        out[f'o{l}'] = ([('out', l, 0)], [f'a{l}{k}' for k in range(BLOCKS)] + [f'd{l}0', f'd{l}1'], 0.6)
    return out


def make_plan():
    groups = [group_parts(*name) for name in SEQUENCE]
    specs = [spec for group in groups for spec in group]
    index = {(g, i): sum(len(h) for h in groups[:g]) + i for g, group in enumerate(groups) for i in range(len(group))}
    events, tasks = arrivals(groups), compute_tasks()
    steps = [(index[g, i], -1) for g in range(WINDOW) for i in range(len(groups[g]))]
    done, left, first_left, set_out, clock = set(), collections.Counter(), collections.Counter(), WINDOW, 0.0
    for g, group in enumerate(groups):
        left[g] = sum(len(spec[4]) + 1 for spec in group)
        first_left[g] = len(group)
    for n, (when, (g, i, phase)) in enumerate(events):
        clock = max(clock, when)
        steps.append((index[g, i], phase))
        left[g] -= 1
        if left[g] == 0:
            done.add(SEQUENCE[g])
        if phase == 0:
            first_left[g] -= 1
            if first_left[g] == 0 and set_out < len(groups):
                steps += [(index[set_out, j], -1) for j in range(len(groups[set_out]))]
                set_out += 1
        until = events[n + 1][0] + SLACK if n + 1 < len(events) else math.inf
        while clock < until:
            ready = [k for k, (needs, after, _) in tasks.items() if done.issuperset(needs) and done.issuperset(after)]
            if not ready:
                break
            steps.append(ready[0])
            done.add(ready[0])
            clock += tasks.pop(ready[0])[2]
    assert not tasks
    return specs, steps


class Part:
    def __init__(self, ref, lead, cols, order, where, sems, held=(Z, Y, X), first=None):
        self.ref, self.lead, self.cols, self.order, self.where = ref, lead, cols, order, where
        self.send_sems, self.recv_sems, self.index = sems
        self.held, self.first = held, first

    def block(self, full, where):
        sel = tuple(pl.ds(0, DIMS[d]) if d in full else where[d] for d in self.held)
        return self.ref.at[self.lead + sel + (where[C], slice(None), self.cols)]

    def device(self, d, value):
        w = list(self.where)
        w[d] = value
        return (((w[0] * 2 + w[1]) * 2 + w[2]) * 2 + w[3],)

    def copies(self, phase):
        d = self.order[phase] if phase < len(self.order) else C
        full = self.order[:phase]
        if self.order[0] == Y and phase > 0 and self.first is not None:
            full = (Y,) + tuple(self.order[1:phase])
        if d == Z:
            targets = [(k, (self.where[Z] + k + 1) % NZ) for k in range(NZ - 1)]
        else:
            targets = [({X: 3, Y: 4, C: 5}[d], 1 - self.where[d])]
        blk = self.block(full, self.where)
        src = self.first if (phase == 0 and self.first is not None) else blk
        return [pltpu.make_async_remote_copy(
            src_ref=src, dst_ref=blk, send_sem=self.send_sems.at[self.index, k], recv_sem=self.recv_sems.at[self.index, k],
            device_id=self.device(d, to), device_id_type=MESH) for k, to in targets]

    @property
    def phases(self):
        return len(self.order) + 1

    def start(self, phase):
        for cp in self.copies(phase):
            cp.start()

    def finish(self, phase):
        for cp in self.copies(phase):
            cp.wait_recv()

    def drain(self):
        for phase in range(self.phases):
            for cp in self.copies(phase):
                cp.wait_send()


def iota(shape, axis):
    return lax.broadcasted_iota(jnp.int32, shape, axis)


def floor_div(values, width):
    return jnp.floor((values + 0.5) * (1.0 / width))


def dot(a, b):
    return jnp.dot(a, b, preferred_element_type=F32)


def layer_norm(x_f32, gain, bias):
    row_mean = jnp.mean(x_f32, axis=-1, keepdims=True)
    centered = x_f32 - row_mean
    row_var = jnp.mean(centered * centered, axis=-1, keepdims=True)
    return (centered * lax.rsqrt(row_var + LN_EPS) * gain + bias).astype(BF16)


def one_hot_cols(width, cols_f32):
    index = cols_f32 - floor_div(cols_f32, width) * width
    return (iota(index.shape, 0).astype(F32) == index).astype(BF16)


def kernel(specs, steps, pos_ref, x_ref, g1_ref, c1_ref, g2_ref, c2_ref, bo_ref, bd_ref, gf_ref, cf_ref, bq_ref, bi_ref, qkv_ref, out_ref, win_ref, down_ref, k_hbm, v_hbm,
           y_ref, kbuf, vbuf,
           vec_g, qkv_g, out_g, win_g, down_g, x1_scr, xn_scr, ps_scr, pr_scr, h1_scr, h2_scr, act_scr, acc_scr,
           rope_ref, pos_scr, vrow_scr, bq_scr, bi_scr, q_scr, kn_scr, vn_scr, ctx_scr, s_scr,
           own_sem, send_sems, recv_sems, xs_sem, xr_sem, ps_sem, pr_sem, in_sem):
    me = lax.axis_index('dp')
    where = (me // 8, (me // 4) % 2, (me // 2) % 2, me % 2)
    z, y, x, c = where

    def device(z, y, x, c):
        return (((z * 2 + y) * 2 + x) * 2 + c,)

    y_peer = device(z, 1 - y, x, c)

    def cache_in(i):
        l, rows = i // BLOCKS, pl.ds(i % BLOCKS * SEQS, SEQS)
        return [pltpu.make_async_copy(k_hbm.at[l, rows], kbuf.at[l, rows], in_sem.at[0, i]),
                pltpu.make_async_copy(v_hbm.at[l, rows], vbuf.at[l, rows], in_sem.at[1, i])]

    def my_cols(zb, yy):
        return pl.ds(pl.multiple_of(768 * zb + 384 * yy, 128), 384)

    own = [(qkv_ref.at[0], qkv_g.at[0, z, y, x, c])]
    own += [(win_ref.at[0, :, my_cols(zb, y)], win_g.at[0, z, y, x, c, :, pl.ds(384 * zb, 384)]) for zb in range(4)]
    own += [(down_ref.at[0], down_g.at[0, z, x, c]), (out_ref.at[0], out_g.at[0, z, y, x, c]), (qkv_ref.at[1], qkv_g.at[1, z, y, x, c])]
    own += [(win_ref.at[1, :, my_cols(zb, y)], win_g.at[1, z, y, x, c, :, pl.ds(384 * zb, 384)]) for zb in range(4)]
    own += [(down_ref.at[1], down_g.at[1, z, x, c]), (out_ref.at[1], out_g.at[1, z, y, x, c])]
    own = [pltpu.make_async_copy(src, dst, own_sem.at[i]) for i, (src, dst) in enumerate(own)]
    for cp in own:
        cp.start()

    barrier = pltpu.get_barrier_semaphore()
    peers = [device((z + k) % NZ, y, x, c) for k in range(1, NZ)] + [device(z, y, 1 - x, c), y_peer, device(z, y, x, 1 - c)]
    for who in peers:
        pl.semaphore_signal(barrier, inc=1, device_id=who, device_id_type=MESH)

    own_vec = vec_g.at[0, z, y, x, c]
    own_vec[...] = jnp.zeros((VEC_ROWS, 128), F32)
    at_row = 0
    for ref in (g1_ref, c1_ref, g2_ref, c2_ref, bo_ref, bd_ref, gf_ref, cf_ref, bq_ref, bi_ref):
        count, width = ref.shape
        own_vec[pl.ds(at_row, count), pl.ds(0, width)] = ref[...].astype(F32)
        at_row += count

    pl.semaphore_wait(barrier, len(peers))
    for cp in own:
        cp.wait()
    for i in range(2 * BLOCKS):
        for cp in cache_in(i):
            cp.start()

    refs = {'vec': vec_g, 'qkv': qkv_g, 'win': win_g, 'down': down_g, 'out': out_g}
    parts = []
    for i, (family, l, col, width, order) in enumerate(specs):
        kw = {}
        if family == 'down':
            kw['held'] = (Z, X)
        if family == 'win':
            kw['first'] = win_ref.at[l, :, my_cols(col // 384, 1 - y)]
        parts.append(Part(refs[family], (l,), pl.ds(col, width), order, where, (send_sems, recv_sems, i), **kw))

    lane = iota((1, 128), 1)

    def send_x(l):
        src = x_ref if l == 0 else x1_scr
        return pltpu.make_async_remote_copy(src_ref=src, dst_ref=xn_scr.at[l], send_sem=xs_sem.at[l], recv_sem=xr_sem.at[l],
                                            device_id=y_peer, device_id_type=MESH)

    def send_part(l):
        return pltpu.make_async_remote_copy(src_ref=ps_scr.at[l], dst_ref=pr_scr.at[l], send_sem=ps_sem.at[l], recv_sem=pr_sem.at[l],
                                            device_id=y_peer, device_id_type=MESH)

    def task_rope():
        for b in range(ROWS):
            pos_scr[pl.ds(b, 1), :] = jnp.full((1, 128), pos_ref[b], jnp.int32).astype(F32)
        d = lane % HEAD
        freq = jnp.zeros((1, 128), F32)
        for i, f in enumerate(FREQS):
            freq = jnp.where(d % 8 == i, f, freq)
        angle = pos_scr[...] * freq
        cos, sin = jnp.cos(angle), jnp.sin(angle)
        for t, turned in enumerate((lane >= 0, lane >= 64, lane < 64)):
            rope_ref[3 * t] = jnp.where(turned & (d < 16), cos, 1.0)
            rope_ref[3 * t + 1] = jnp.where(turned & (d < 8), -sin, 0.0)
            rope_ref[3 * t + 2] = jnp.where(turned & (d >= 8) & (d < 16), sin, 0.0)

    def task_vec():
        vec2 = vec_g[...].reshape(32 * VEC_ROWS, 128).astype(BF16)
        n = iota((1, D), 1).astype(F32)
        spread = dot(vec2, one_hot_cols(24, jnp.broadcast_to(n, (128, D))))
        r = iota((32 * VEC_ROWS, 1), 0).astype(F32)
        mine = floor_div(n, 24) == floor_div(r, VEC_ROWS)
        spread = jnp.where(mine, spread, 0.0).astype(BF16)
        rr = iota((1, 32 * VEC_ROWS), 1).astype(F32)
        kind = rr - floor_div(rr, VEC_ROWS) * VEC_ROWS
        pick = (iota((VEC_ROWS, 32 * VEC_ROWS), 0).astype(F32) == kind).astype(BF16)
        vrow_scr[...] = dot(pick, spread)
        dev = iota((32, 1), 0).astype(F32)

        def long_row(kind, width, cols):
            g = vec_g[0, :, :, :, :, kind].reshape(32, 128).astype(BF16)
            n = cols.astype(F32)
            full = dot(g, one_hot_cols(width, jnp.broadcast_to(n, (128, n.shape[1]))))
            return jnp.sum(jnp.where(floor_div(n, width) == dev, full, 0.0), axis=0, keepdims=True)

        for l in range(2):
            bq_scr[l] = long_row(14 + l, 72, iota((1, 3 * D), 1))
            for zb in range(4):
                bi_scr[l, :, pl.ds(384 * zb, 384)] = long_row(16 + l, 96, iota((1, 384), 1) + (768 * zb + 384 * y))

    def vrow(kind):
        return vrow_scr[pl.ds(kind, 1), :]

    def x_of(l):
        return (x_ref if l == 0 else x1_scr)[...]

    def task_start(l):
        send_x(l).start()
        h1_scr[...] = layer_norm(x_of(l).astype(F32), vrow(l), vrow(2 + l))

    def task_qkv(l, i):
        w = qkv_g[l, :, :, :, :, :, pl.ds(768 * i, 768)].reshape(D, 768)
        got = (dot(h1_scr[...], w) + bq_scr[l, :, pl.ds(768 * i, 768)]).astype(BF16).astype(F32)
        for m in range(2):
            tiles = []
            for t in range(3):
                v = got[:, 384 * m + 128 * t: 384 * m + 128 * t + 128]
                r = v * rope_ref[3 * t] + pltpu.roll(v, 120, 1) * rope_ref[3 * t + 1] + pltpu.roll(v, 8, 1) * rope_ref[3 * t + 2]
                tiles.append(r.astype(BF16).astype(F32))
            h = 4 * i + 2 * m
            t0, t1, t2 = tiles
            q_scr[pl.ds(h, ROWS, stride=16), :] = t0
            kn_scr[pl.ds(h, ROWS, stride=16), :] = pltpu.roll(t0, 64, 1)
            vn_scr[pl.ds(h, ROWS, stride=16), :] = t1
            q_scr[pl.ds(h + 1, ROWS, stride=16), :] = pltpu.roll(t1, 64, 1)
            kn_scr[pl.ds(h + 1, ROWS, stride=16), :] = t2
            vn_scr[pl.ds(h + 1, ROWS, stride=16), :] = pltpu.roll(t2, 64, 1)

    def task_att(l, blk):
        for cp in cache_in(l * BLOCKS + blk):
            cp.wait()
        key = iota((1, KEYS), 1)
        head_row = jnp.minimum(iota((16, 1), 0), HEADS - 1) * SLOTS
        slot_of = key - head_row
        own_head = (slot_of >= 0) & (slot_of < SLOTS)
        slots = iota((SLOTS, HEAD), 0)

        def scores(j):
            b = blk * SEQS + j
            pos = pos_ref[b]
            rows = pl.ds(b * 16, 16)
            put = jnp.where(slots == pos, 1.0, 0.0).astype(BF16) > 0.5

            def placed(buf, new_scr):
                new = new_scr[rows, :][:HEADS, :HEAD].astype(BF16)
                both = jnp.where(put[None], new[:, None, :], buf[l, blk * SEQS + j])
                buf[l, blk * SEQS + j] = both
                return both.reshape(KEYS, HEAD)

            keys = placed(kbuf, kn_scr)
            placed(vbuf, vn_scr)
            q = q_scr[rows, :][:, :HEAD].astype(BF16)
            s = lax.dot_general(q, keys, (((1,), (1,)), ((), ())), preferred_element_type=F32) * (HEAD ** -0.5)
            s_scr[pl.ds(j * 16, 16), :] = jnp.where(own_head & (slot_of <= pos), s, -jnp.inf)

        def weighted(j):
            p = s_scr[pl.ds(j * 16, 16), :].astype(BF16)
            got = dot(p, vbuf[l, blk * SEQS + j].reshape(KEYS, HEAD))
            ctx_scr[pl.ds((blk * SEQS + j) * 16, 16), pl.ds(0, HEAD)] = got

        for j in range(SEQS):
            scores(j)
        s = s_scr[...]
        e = jnp.exp(s - jnp.max(s, axis=-1, keepdims=True))
        s_scr[...] = e / jnp.sum(e, axis=-1, keepdims=True)
        for j in range(SEQS):
            weighted(j)

    def task_h2(l):
        send_x(l).wait_recv()
        for half, v in enumerate((x_of(l), xn_scr[l])):
            h2_scr[pl.ds(ROWS * half, ROWS), :] = layer_norm(v.astype(F32), vrow(4 + l), vrow(6 + l))

    def task_win(l, zb):
        cols = pl.ds(384 * zb, 384)
        w = win_g[l, :, :, :, :, :, cols].reshape(D, 384)
        u = dot(h2_scr[...], w) + bi_scr[l, :, cols]
        act_scr[:, cols] = (0.5 * u * (1.0 + lax.erf(u * 0.7071067811865476))).astype(BF16)

    def task_down(l, i):
        cols = pl.ds(384 * i, 384)
        got = dot(act_scr[...], down_g[l, :, :, :, :, cols].reshape(HID, 384))
        acc_scr[:, cols] = got[:ROWS]
        ps_scr[l, :, cols] = got[ROWS:]
        if i == 1:
            send_part(l).start()

    def task_out(l):
        tiles = []
        for m in range(HEADS // 2):
            a = ctx_scr[pl.ds(2 * m, ROWS, stride=16), :]
            b = pltpu.roll(ctx_scr[pl.ds(2 * m + 1, ROWS, stride=16), :], 64, 1)
            tiles.append(jnp.where(lane < 64, a, b).astype(BF16))
        a = dot(jnp.concatenate(tiles, axis=1), out_g[l].reshape(D, D)) + vrow(8 + l)
        send_part(l).wait_recv()
        m = acc_scr[...] + pr_scr[l] + vrow(10 + l)
        new = (x_of(l).astype(F32) + a + m).astype(BF16)
        if l == 0:
            x1_scr[...] = new
        else:
            y_ref[...] = layer_norm(new.astype(F32), vrow(12), vrow(13))

    tasks = {'vec': task_vec}
    for l in range(2):
        tasks[f's{l}'] = functools.partial(task_start, l)
        tasks[f'h{l}'] = functools.partial(task_h2, l)
        tasks[f'o{l}'] = functools.partial(task_out, l)
        for name, fn, count in (('q', task_qkv, 3), ('w', task_win, 4), ('d', task_down, 2), ('a', task_att, BLOCKS)):
            for i in range(count):
                tasks[f'{name}{l}{i}'] = functools.partial(fn, l, i)

    for n, step in enumerate(steps):
        if isinstance(step, str):
            tasks.pop(step)()
            continue
        p, phase = parts[step[0]], step[1]
        if phase >= 0:
            p.finish(phase)
        if phase + 1 < p.phases:
            p.start(phase + 1)
        if n == FIRST:
            task_rope()
    assert not tasks

    for p in parts:
        p.drain()
    for l in range(2):
        send_x(l).wait_send()
        send_part(l).wait_send()


def write_kernel(y_ref, k_ref, v_ref, y_hbm, k_hbm, v_hbm, sem):
    copies = [pltpu.make_async_copy(y_ref, y_hbm, sem.at[0])]
    for ref, hbm in ((k_ref, k_hbm), (v_ref, v_hbm)):
        for l in range(2):
            for i in range(4):
                rows = pl.ds(16 * i, 16)
                copies.append(pltpu.make_async_copy(ref.at[l, rows], hbm.at[l, rows], sem.at[len(copies)]))
    for cp in copies:
        cp.start()
    for cp in copies:
        cp.wait()


def fused(pos, x, vecs, w_qkv, w_out, w_in, w_down, k_cache, v_cache):
    specs, steps = make_plan()
    parts = len(specs)
    vmem = pl.BlockSpec(memory_space=pltpu.VMEM)
    hbm = pl.BlockSpec(memory_space=pl.ANY)
    lead = (4, 2, 2, 2)
    dma = pltpu.SemaphoreType.DMA
    outs = (x, k_cache, v_cache)
    y, k_new, v_new = pl.pallas_call(
        functools.partial(kernel, specs, steps),
        out_shape=tuple(pltpu.VMEM(a.shape, a.dtype) for a in outs),
        in_specs=[pl.BlockSpec(memory_space=pltpu.SMEM), vmem] + [vmem] * len(vecs) + [hbm] * 6,
        out_specs=[vmem] * 3,
        scratch_shapes=[
            pltpu.VMEM((1,) + lead + (VEC_ROWS, 128), F32),
            pltpu.VMEM((2,) + lead + (24, 3 * D), BF16),
            pltpu.VMEM((2,) + lead + (24, D), BF16),
            pltpu.VMEM((2,) + lead + (24, HID), BF16),
            pltpu.VMEM((2, 4, 2, 2, 96, D), BF16),
            pltpu.VMEM((ROWS, D), BF16),
            pltpu.VMEM((2, ROWS, D), BF16),
            pltpu.VMEM((2, ROWS, D), F32),
            pltpu.VMEM((2, ROWS, D), F32),
            pltpu.VMEM((ROWS, D), BF16),
            pltpu.VMEM((2 * ROWS, D), BF16),
            pltpu.VMEM((2 * ROWS, HID), BF16),
            pltpu.VMEM((ROWS, D), F32),
            pltpu.VMEM((9, ROWS, 128), F32),
            pltpu.VMEM((ROWS, 128), F32),
            pltpu.VMEM((VEC_ROWS, D), F32),
            pltpu.VMEM((2, 1, 3 * D), F32),
            pltpu.VMEM((2, 1, HID), F32),
            pltpu.VMEM((16 * ROWS, 128), F32),
            pltpu.VMEM((16 * ROWS, 128), F32),
            pltpu.VMEM((16 * ROWS, 128), F32),
            pltpu.VMEM((16 * ROWS, 128), F32),
            pltpu.VMEM((16 * SEQS, KEYS), F32),
            dma((16,)), dma((parts, SENDS)), dma((parts, SENDS)), dma((2,)), dma((2,)), dma((2,)), dma((2,)), dma((2, 2 * BLOCKS)),
        ],
        compiler_params=pltpu.CompilerParams(collective_id=0, has_side_effects=True, vmem_limit_bytes=VMEM_LIMIT),
    )(pos, x, *vecs, w_qkv, w_out, w_in, w_down, k_cache, v_cache)
    return pl.pallas_call(
        write_kernel,
        out_shape=tuple(jax.ShapeDtypeStruct(a.shape, a.dtype) for a in outs),
        in_specs=[vmem] * 3,
        out_specs=[hbm] * 3,
        scratch_shapes=[dma((17,))],
        compiler_params=pltpu.CompilerParams(vmem_limit_bytes=VMEM_SMALL),
    )(y, k_new, v_new)


def solution(mesh):
    row_spec = P('dp', None)
    vec_spec = P(None, 'dp')
    mat_spec = P(None, 'dp', None)
    cache_spec = P(None, 'dp', None, None, None)
    in_specs = (row_spec, P('dp'), cache_spec, cache_spec, vec_spec, vec_spec, vec_spec, vec_spec, mat_spec, vec_spec, mat_spec, vec_spec, mat_spec, vec_spec, mat_spec, vec_spec, P('dp'), P('dp'))
    out_specs = (row_spec, cache_spec, cache_spec)

    def device_step(x_embed, positions, k_cache, v_cache, ln1_gain, ln1_bias, ln2_gain, ln2_bias, w_qkv, b_qkv, w_out, b_out, w_in, b_in, w_down, b_down, lnf_gain, lnf_bias):
        vecs = (ln1_gain, ln1_bias, ln2_gain, ln2_bias, b_out, b_down, lnf_gain[None], lnf_bias[None], b_qkv, b_in)
        by_head = lambda a: jnp.swapaxes(a, 2, 3)
        out, k_new, v_new = fused(positions, x_embed, vecs, w_qkv, w_out, w_in, w_down, by_head(k_cache), by_head(v_cache))
        return out, by_head(k_new), by_head(v_new)

    return jax.shard_map(device_step, mesh=mesh, in_specs=in_specs, out_specs=out_specs, check_vma=False)
```

```python
import collections
import functools
import heapq
import itertools
import math
import jax
import jax.numpy as jnp
import numpy as np
from jax import lax
from jax.experimental import pallas as pl
from jax.experimental.pallas import tpu as pltpu
from jax.sharding import PartitionSpec as P

LN_EPS = 1e-5
ROPE_BASE = 10000.0
MESH = pl.DeviceIdType.MESH
F32, BF16 = jnp.float32, jnp.bfloat16
NZ = 4
Z, Y, X, C = 0, 1, 2, 3
Z1, Z2, Z3 = 4, 5, 6
ALONG_Z = (Z1, Z2, Z3)
DIMS = (4, 2, 2, 2)
VEC_ROWS = 24
ROWS, D, HEADS, HEAD, SLOTS, FF = 64, 768, 12, 64, 32, 3072
KEYS = HEADS * SLOTS
HID = FF // 2
SEQS = 8
BLOCKS = ROWS // SEQS
VMEM_LIMIT, VMEM_SMALL = 36 << 20, 1 << 20
FREQS = tuple(float(np.float32(1.0) / np.float32(ROPE_BASE) ** (np.float32(2 * i) / np.float32(16))) for i in range(8))
FIRST = 7
SENDS = 9


LINK, CORES = 46600.0, 300000.0
FIXED, FIXED_CORES = 1.6, 0.9
WINDOW, SLACK = 3, -0.5
ZXY, ZYX, XYZ, YXZ = ALONG_Z + (X, Y), ALONG_Z + (Y, X), (X, Y) + ALONG_Z, (Y, X) + ALONG_Z
YZX, ZX, XZ = (Y,) + ALONG_Z + (X,), ALONG_Z + (X,), (X,) + ALONG_Z
SHARES = {
    'vec': [((1, ZXY),)],
    'qkv': [((3, ZXY), (3, ZYX)), ((6, ZXY),)],
    'out': [((6, ZXY),), ((6, ZXY),)],
    'win': [((3, YZX),)] * 2,
    'down': [((2, ZX), (1, XZ))] * 2,
}
GROUPS = tuple((f, l, i) for f, layers, n in (('vec', 1, 1), ('qkv', 2, 3), ('win', 2, 4), ('down', 2, 2), ('out', 2, 1)) for l in range(layers) for i in range(n))
SEQUENCE = tuple(GROUPS[ord(k) - ord('a')] for k in 'cbaegqldhijfktnospmur')


def group_parts(family, l, i):
    out, at = [], {'qkv': D, 'win': HID // 4, 'down': D // 2}.get(family, 0) * i
    for units, order in SHARES[family][l]:
        out.append((family, l, at, units * 128, order))
        at += units * 128
    return out


def gathered(order, phase):
    return {Z if d == Z3 else d for d in order[:phase]} - {Z1, Z2}


def sends(spec, phase, chip):
    family, _, _, width, order = spec
    size, z = width * {'vec': VEC_ROWS * 4, 'down': 192}.get(family, 48), chip[Z]
    for d in gathered(order, phase):
        size *= DIMS[d]
    if phase == len(order):
        return [(chip, size, chip)]
    axis = order[phase]
    if axis in ALONG_Z:
        hop, out = axis - Z1, []
        if hop <= z < NZ - 1:
            out.append(((z + 1,) + chip[1:], size, (Z, True) + chip))
        if 0 < z < NZ - hop:
            out.append(((z - 1,) + chip[1:], size, (Z, False) + chip))
        return out
    to = tuple(1 - v if e == axis else v for e, v in enumerate(chip))
    return [(to, size, (axis,) + chip)]


def comes(order, phase, chip):
    if phase == len(order) or order[phase] not in ALONG_Z:
        return 1
    hop = order[phase] - Z1
    return (chip[Z] > hop) + (chip[Z] + hop + 1 < NZ)


def arrivals(groups):
    chips = list(itertools.product(range(4), range(2), range(2)))
    free, heap, got, at, times = {}, [], collections.Counter(), collections.Counter(), collections.defaultdict(list)
    set_out, ticket = {chip: WINDOW for chip in chips}, itertools.count()

    def send(now, chip, g, i, phase):
        for to, size, link in sends(groups[g][i], phase, chip):
            own = to == chip
            free[link] = max(now, free.get(link, 0.0)) + size / (CORES if own else LINK)
            heapq.heappush(heap, (free[link] + (FIXED_CORES if own else FIXED), next(ticket), to, g, i, phase))

    for chip in chips:
        for g in range(WINDOW):
            for i in range(len(groups[g])):
                send(0.0, chip, g, i, 0)
    while heap:
        now, _, chip, g, i, phase = heapq.heappop(heap)
        got[chip, g, i, phase] += 1
        order = groups[g][i][4]
        while at[chip, g, i] <= len(order) and got[chip, g, i, at[chip, g, i]] == comes(order, at[chip, g, i], chip):
            over = at[chip, g, i]
            times[g, i, over].append(now)
            at[chip, g, i] += 1
            if over < len(order):
                send(now, chip, g, i, over + 1)
            if over == 0:
                got[chip, g] += 1
                if got[chip, g] == len(groups[g]) and set_out[chip] < len(groups):
                    later = set_out[chip]
                    set_out[chip] += 1
                    for j in range(len(groups[later])):
                        send(now, chip, later, j, 0)
    mean = {k: sum(v) / len(v) for k, v in times.items()}
    for g, i, phase in sorted(mean):
        if phase:
            mean[g, i, phase] = max(mean[g, i, phase], mean[g, i, phase - 1])
    return sorted((v, k) for k, v in mean.items())


def compute_tasks():
    out = {'vec': ([('vec', 0, 0)], [], 2.0)}
    for l in range(2):
        out[f's{l}'] = ([], ['o0'] if l else ['vec'], 0.3)
        for i in range(3):
            out[f'q{l}{i}'] = ([('qkv', l, i)], [f's{l}'], 0.6)
        out[f'h{l}'] = ([], [f'q{l}2'], 0.5)
        for i in range(4):
            out[f'w{l}{i}'] = ([('win', l, i)], [f'h{l}'], 0.5)
        for i in range(2):
            out[f'd{l}{i}'] = ([('down', l, i)], [f'w{l}{k}' for k in range(4)], 0.5)
        for i in range(BLOCKS):
            out[f'a{l}{i}'] = ([], [f'q{l}{k}' for k in range(3)], 1.2)
        out[f'o{l}'] = ([('out', l, 0)], [f'a{l}{k}' for k in range(BLOCKS)] + [f'd{l}0', f'd{l}1'], 0.6)
    return out


def make_plan():
    groups = [group_parts(*name) for name in SEQUENCE]
    specs = [spec for group in groups for spec in group]
    index = {(g, i): sum(len(h) for h in groups[:g]) + i for g, group in enumerate(groups) for i in range(len(group))}
    events, tasks = arrivals(groups), compute_tasks()
    steps = [(index[g, i], -1) for g in range(WINDOW) for i in range(len(groups[g]))]
    done, left, first_left, set_out, clock = set(), collections.Counter(), collections.Counter(), WINDOW, 0.0
    for g, group in enumerate(groups):
        left[g] = sum(len(spec[4]) + 1 for spec in group)
        first_left[g] = len(group)
    for n, (when, (g, i, phase)) in enumerate(events):
        clock = max(clock, when)
        steps.append((index[g, i], phase))
        left[g] -= 1
        if left[g] == 0:
            done.add(SEQUENCE[g])
        if phase == 0:
            first_left[g] -= 1
            if first_left[g] == 0 and set_out < len(groups):
                steps += [(index[set_out, j], -1) for j in range(len(groups[set_out]))]
                set_out += 1
        until = events[n + 1][0] + SLACK if n + 1 < len(events) else math.inf
        while clock < until:
            ready = [k for k, (needs, after, _) in tasks.items() if done.issuperset(needs) and done.issuperset(after)]
            if not ready:
                break
            steps.append(ready[0])
            done.add(ready[0])
            clock += tasks.pop(ready[0])[2]
    assert not tasks
    return specs, steps


class Part:
    def __init__(self, ref, lead, cols, order, where, sems, held=(Z, Y, X), first=None):
        self.ref, self.lead, self.cols, self.order, self.where = ref, lead, cols, order, where
        self.send_sems, self.recv_sems, self.index = sems
        self.held, self.first = held, first

    def copy(self, phase, axis, to, slot, z):
        full = gathered(self.order, phase)
        if self.first is not None and phase > 0:
            full.add(Y)
        at = (z,) + self.where[1:]
        sel = tuple(pl.ds(0, DIMS[d]) if d in full else at[d] for d in self.held)
        blk = self.ref.at[self.lead + sel + (self.where[C], slice(None), self.cols)]
        w = list(self.where)
        w[axis] = to
        return pltpu.make_async_remote_copy(
            src_ref=self.first if phase == 0 and self.first is not None else blk, dst_ref=blk,
            send_sem=self.send_sems.at[self.index, slot], recv_sem=self.recv_sems.at[self.index, slot],
            device_id=((((w[0] * 2 + w[1]) * 2 + w[2]) * 2 + w[3]),), device_id_type=MESH)

    def copies(self, phase, mine):
        axis, z = self.order[phase] if phase < len(self.order) else C, self.where[Z]
        if axis not in ALONG_Z:
            return [(None, self.copy(phase, axis, 1 - self.where[axis], {X: 6, Y: 7, C: 8}[axis], z))]
        hop = axis - Z1
        if mine:
            return [((z >= hop) & (z < NZ - 1), self.copy(phase, Z, z + 1, hop, z - hop)),
                    ((z + hop < NZ) & (z > 0), self.copy(phase, Z, z - 1, 3 + hop, z + hop))]
        return [(z > hop, self.copy(phase, Z, z, hop, z - hop - 1)), (z + hop + 1 < NZ, self.copy(phase, Z, z, 3 + hop, z + hop + 1))]

    @property
    def phases(self):
        return len(self.order) + 1

    def each(self, phase, mine, act):
        for condition, cp in self.copies(phase, mine):
            if condition is None:
                act(cp)
            else:
                pl.when(condition)(functools.partial(act, cp))

    def start(self, phase):
        self.each(phase, True, lambda cp: cp.start())

    def finish(self, phase):
        self.each(phase, False, lambda cp: cp.wait_recv())

    def drain(self):
        for phase in range(self.phases):
            self.each(phase, True, lambda cp: cp.wait_send())


def iota(shape, axis):
    return lax.broadcasted_iota(jnp.int32, shape, axis)


def floor_div(values, width):
    return jnp.floor((values + 0.5) * (1.0 / width))


def dot(a, b):
    return jnp.dot(a, b, preferred_element_type=F32)


def layer_norm(x_f32, gain, bias):
    row_mean = jnp.mean(x_f32, axis=-1, keepdims=True)
    centered = x_f32 - row_mean
    row_var = jnp.mean(centered * centered, axis=-1, keepdims=True)
    return (centered * lax.rsqrt(row_var + LN_EPS) * gain + bias).astype(BF16)


def one_hot_cols(width, cols_f32):
    index = cols_f32 - floor_div(cols_f32, width) * width
    return (iota(index.shape, 0).astype(F32) == index).astype(BF16)


def kernel(specs, steps, pos_ref, x_ref, g1_ref, c1_ref, g2_ref, c2_ref, bo_ref, bd_ref, gf_ref, cf_ref, bq_ref, bi_ref, qkv_ref, out_ref, win_ref, down_ref, k_hbm, v_hbm,
           y_ref, kbuf, vbuf,
           vec_g, qkv_g, out_g, win_g, down_g, x1_scr, xn_scr, ps_scr, pr_scr, h1_scr, h2_scr, act_scr, acc_scr,
           rope_ref, pos_scr, vrow_scr, bq_scr, bi_scr, q_scr, kn_scr, vn_scr, ctx_scr, s_scr,
           own_sem, send_sems, recv_sems, xs_sem, xr_sem, ps_sem, pr_sem, in_sem):
    me = lax.axis_index('dp')
    where = (me // 8, (me // 4) % 2, (me // 2) % 2, me % 2)
    z, y, x, c = where

    def device(z, y, x, c):
        return (((z * 2 + y) * 2 + x) * 2 + c,)

    y_peer = device(z, 1 - y, x, c)

    def cache_in(i):
        l, rows = i // BLOCKS, pl.ds(i % BLOCKS * SEQS, SEQS)
        return [pltpu.make_async_copy(k_hbm.at[l, rows], kbuf.at[l, rows], in_sem.at[0, i]),
                pltpu.make_async_copy(v_hbm.at[l, rows], vbuf.at[l, rows], in_sem.at[1, i])]

    def my_cols(zb, yy):
        return pl.ds(pl.multiple_of(768 * zb + 384 * yy, 128), 384)

    own = [(qkv_ref.at[0], qkv_g.at[0, z, y, x, c])]
    own += [(win_ref.at[0, :, my_cols(zb, y)], win_g.at[0, z, y, x, c, :, pl.ds(384 * zb, 384)]) for zb in range(4)]
    own += [(down_ref.at[0], down_g.at[0, z, x, c]), (out_ref.at[0], out_g.at[0, z, y, x, c]), (qkv_ref.at[1], qkv_g.at[1, z, y, x, c])]
    own += [(win_ref.at[1, :, my_cols(zb, y)], win_g.at[1, z, y, x, c, :, pl.ds(384 * zb, 384)]) for zb in range(4)]
    own += [(down_ref.at[1], down_g.at[1, z, x, c]), (out_ref.at[1], out_g.at[1, z, y, x, c])]
    own = [pltpu.make_async_copy(src, dst, own_sem.at[i]) for i, (src, dst) in enumerate(own)]
    for cp in own:
        cp.start()

    barrier = pltpu.get_barrier_semaphore()
    for who in (device(z, y, 1 - x, c), y_peer, device(z, y, x, 1 - c)):
        pl.semaphore_signal(barrier, inc=1, device_id=who, device_id_type=MESH)
    for there, step in ((z > 0, -1), (z < NZ - 1, 1)):
        @pl.when(there)
        def _(step=step):
            pl.semaphore_signal(barrier, inc=1, device_id=device(z + step, y, x, c), device_id_type=MESH)
    own_vec = vec_g.at[0, z, y, x, c]
    own_vec[...] = jnp.zeros((VEC_ROWS, 128), F32)
    at_row = 0
    for ref in (g1_ref, c1_ref, g2_ref, c2_ref, bo_ref, bd_ref, gf_ref, cf_ref, bq_ref, bi_ref):
        count, width = ref.shape
        own_vec[pl.ds(at_row, count), pl.ds(0, width)] = ref[...].astype(F32)
        at_row += count

    pl.semaphore_wait(barrier, 3 + (z + 3) // 4 + (6 - z) // 4)
    for cp in own:
        cp.wait()
    for i in range(2 * BLOCKS):
        for cp in cache_in(i):
            cp.start()

    refs = {'vec': vec_g, 'qkv': qkv_g, 'win': win_g, 'down': down_g, 'out': out_g}
    parts = []
    for i, (family, l, col, width, order) in enumerate(specs):
        kw = {}
        if family == 'down':
            kw['held'] = (Z, X)
        if family == 'win':
            kw['first'] = win_ref.at[l, :, pl.ds(pl.multiple_of(768 * (col // 384) + 384 * (1 - y) + col % 384, 128), width)]
        parts.append(Part(refs[family], (l,), pl.ds(col, width), order, where, (send_sems, recv_sems, i), **kw))

    lane = iota((1, 128), 1)

    def send_x(l):
        src = x_ref if l == 0 else x1_scr
        return pltpu.make_async_remote_copy(src_ref=src, dst_ref=xn_scr.at[l], send_sem=xs_sem.at[l], recv_sem=xr_sem.at[l],
                                            device_id=y_peer, device_id_type=MESH)

    def send_part(l, i):
        cols = pl.ds(384 * i, 384)
        return pltpu.make_async_remote_copy(src_ref=ps_scr.at[l, :, cols], dst_ref=pr_scr.at[l, :, cols], send_sem=ps_sem.at[l, i],
                                            recv_sem=pr_sem.at[l, i], device_id=y_peer, device_id_type=MESH)

    def task_rope():
        for b in range(ROWS):
            pos_scr[pl.ds(b, 1), :] = jnp.full((1, 128), pos_ref[b], jnp.int32).astype(F32)
        d = lane % HEAD
        freq = jnp.zeros((1, 128), F32)
        for i, f in enumerate(FREQS):
            freq = jnp.where(d % 8 == i, f, freq)
        angle = pos_scr[...] * freq
        cos, sin = jnp.cos(angle), jnp.sin(angle)
        for t, turned in enumerate((lane >= 0, lane >= 64, lane < 64)):
            rope_ref[3 * t] = jnp.where(turned & (d < 16), cos, 1.0)
            rope_ref[3 * t + 1] = jnp.where(turned & (d < 8), -sin, 0.0)
            rope_ref[3 * t + 2] = jnp.where(turned & (d >= 8) & (d < 16), sin, 0.0)

    def task_vec():
        vec2 = vec_g[...].reshape(32 * VEC_ROWS, 128).astype(BF16)
        n = iota((1, D), 1).astype(F32)
        spread = dot(vec2, one_hot_cols(24, jnp.broadcast_to(n, (128, D))))
        r = iota((32 * VEC_ROWS, 1), 0).astype(F32)
        mine = floor_div(n, 24) == floor_div(r, VEC_ROWS)
        spread = jnp.where(mine, spread, 0.0).astype(BF16)
        rr = iota((1, 32 * VEC_ROWS), 1).astype(F32)
        kind = rr - floor_div(rr, VEC_ROWS) * VEC_ROWS
        pick = (iota((VEC_ROWS, 32 * VEC_ROWS), 0).astype(F32) == kind).astype(BF16)
        vrow_scr[...] = dot(pick, spread)
        dev = iota((32, 1), 0).astype(F32)

        def long_row(kind, width, cols):
            g = vec_g[0, :, :, :, :, kind].reshape(32, 128).astype(BF16)
            n = cols.astype(F32)
            full = dot(g, one_hot_cols(width, jnp.broadcast_to(n, (128, n.shape[1]))))
            return jnp.sum(jnp.where(floor_div(n, width) == dev, full, 0.0), axis=0, keepdims=True)

        for l in range(2):
            bq_scr[l] = long_row(14 + l, 72, iota((1, 3 * D), 1))
            for zb in range(4):
                bi_scr[l, :, pl.ds(384 * zb, 384)] = long_row(16 + l, 96, iota((1, 384), 1) + (768 * zb + 384 * y))

    def vrow(kind):
        return vrow_scr[pl.ds(kind, 1), :]

    def x_of(l):
        return (x_ref if l == 0 else x1_scr)[...]

    def task_start(l):
        send_x(l).start()
        h1_scr[...] = layer_norm(x_of(l).astype(F32), vrow(l), vrow(2 + l))

    def task_qkv(l, i):
        w = qkv_g[l, :, :, :, :, :, pl.ds(768 * i, 768)].reshape(D, 768)
        got = (dot(h1_scr[...], w) + bq_scr[l, :, pl.ds(768 * i, 768)]).astype(BF16).astype(F32)
        for m in range(2):
            tiles = []
            for t in range(3):
                v = got[:, 384 * m + 128 * t: 384 * m + 128 * t + 128]
                r = v * rope_ref[3 * t] + pltpu.roll(v, 120, 1) * rope_ref[3 * t + 1] + pltpu.roll(v, 8, 1) * rope_ref[3 * t + 2]
                tiles.append(r.astype(BF16).astype(F32))
            h = 4 * i + 2 * m
            t0, t1, t2 = tiles
            q_scr[pl.ds(h, ROWS, stride=16), :] = t0
            kn_scr[pl.ds(h, ROWS, stride=16), :] = pltpu.roll(t0, 64, 1)
            vn_scr[pl.ds(h, ROWS, stride=16), :] = t1
            q_scr[pl.ds(h + 1, ROWS, stride=16), :] = pltpu.roll(t1, 64, 1)
            kn_scr[pl.ds(h + 1, ROWS, stride=16), :] = t2
            vn_scr[pl.ds(h + 1, ROWS, stride=16), :] = pltpu.roll(t2, 64, 1)

    def task_att(l, blk):
        for cp in cache_in(l * BLOCKS + blk):
            cp.wait()
        key = iota((1, KEYS), 1)
        head_row = jnp.minimum(iota((16, 1), 0), HEADS - 1) * SLOTS
        slot_of = key - head_row
        own_head = (slot_of >= 0) & (slot_of < SLOTS)
        slots = iota((SLOTS, HEAD), 0)

        def scores(j):
            b = blk * SEQS + j
            pos = pos_ref[b]
            rows = pl.ds(b * 16, 16)
            put = jnp.where(slots == pos, 1.0, 0.0).astype(BF16) > 0.5

            def placed(buf, new_scr):
                new = new_scr[rows, :][:HEADS, :HEAD].astype(BF16)
                both = jnp.where(put[None], new[:, None, :], buf[l, blk * SEQS + j])
                buf[l, blk * SEQS + j] = both
                return both.reshape(KEYS, HEAD)

            keys = placed(kbuf, kn_scr)
            placed(vbuf, vn_scr)
            q = q_scr[rows, :][:, :HEAD].astype(BF16)
            s = lax.dot_general(q, keys, (((1,), (1,)), ((), ())), preferred_element_type=F32) * (HEAD ** -0.5)
            s_scr[pl.ds(j * 16, 16), :] = jnp.where(own_head & (slot_of <= pos), s, -jnp.inf)

        def weighted(j):
            p = s_scr[pl.ds(j * 16, 16), :].astype(BF16)
            got = dot(p, vbuf[l, blk * SEQS + j].reshape(KEYS, HEAD))
            ctx_scr[pl.ds((blk * SEQS + j) * 16, 16), pl.ds(0, HEAD)] = got

        for j in range(SEQS):
            scores(j)
        s = s_scr[...]
        e = jnp.exp(s - jnp.max(s, axis=-1, keepdims=True))
        s_scr[...] = e / jnp.sum(e, axis=-1, keepdims=True)
        for j in range(SEQS):
            weighted(j)

    def task_h2(l):
        send_x(l).wait_recv()
        for half, v in enumerate((x_of(l), xn_scr[l])):
            h2_scr[pl.ds(ROWS * half, ROWS), :] = layer_norm(v.astype(F32), vrow(4 + l), vrow(6 + l))

    def task_win(l, zb):
        cols = pl.ds(384 * zb, 384)
        w = win_g[l, :, :, :, :, :, cols].reshape(D, 384)
        u = dot(h2_scr[...], w) + bi_scr[l, :, cols]
        act_scr[:, cols] = (0.5 * u * (1.0 + lax.erf(u * 0.7071067811865476))).astype(BF16)

    def task_down(l, i):
        cols = pl.ds(384 * i, 384)
        got = dot(act_scr[...], down_g[l, :, :, :, :, cols].reshape(HID, 384))
        acc_scr[:, cols] = got[:ROWS]
        ps_scr[l, :, cols] = got[ROWS:]
        send_part(l, i).start()

    def task_out(l):
        tiles = []
        for m in range(HEADS // 2):
            a = ctx_scr[pl.ds(2 * m, ROWS, stride=16), :]
            b = pltpu.roll(ctx_scr[pl.ds(2 * m + 1, ROWS, stride=16), :], 64, 1)
            tiles.append(jnp.where(lane < 64, a, b).astype(BF16))
        a = dot(jnp.concatenate(tiles, axis=1), out_g[l].reshape(D, D)) + vrow(8 + l)
        for i in range(2):
            send_part(l, i).wait_recv()
        m = acc_scr[...] + pr_scr[l] + vrow(10 + l)
        new = (x_of(l).astype(F32) + a + m).astype(BF16)
        if l == 0:
            x1_scr[...] = new
        else:
            y_ref[...] = layer_norm(new.astype(F32), vrow(12), vrow(13))

    tasks = {'vec': task_vec}
    for l in range(2):
        tasks[f's{l}'] = functools.partial(task_start, l)
        tasks[f'h{l}'] = functools.partial(task_h2, l)
        tasks[f'o{l}'] = functools.partial(task_out, l)
        for name, fn, count in (('q', task_qkv, 3), ('w', task_win, 4), ('d', task_down, 2), ('a', task_att, BLOCKS)):
            for i in range(count):
                tasks[f'{name}{l}{i}'] = functools.partial(fn, l, i)

    for n, step in enumerate(steps):
        if isinstance(step, str):
            tasks.pop(step)()
            continue
        p, phase = parts[step[0]], step[1]
        if phase >= 0:
            p.finish(phase)
        if phase + 1 < p.phases:
            p.start(phase + 1)
        if n == FIRST:
            task_rope()
    assert not tasks

    for p in parts:
        p.drain()
    for l in range(2):
        send_x(l).wait_send()
        for i in range(2):
            send_part(l, i).wait_send()


def write_kernel(y_ref, k_ref, v_ref, y_hbm, k_hbm, v_hbm, sem):
    copies = [pltpu.make_async_copy(y_ref, y_hbm, sem.at[0])]
    for ref, hbm in ((k_ref, k_hbm), (v_ref, v_hbm)):
        for l in range(2):
            for i in range(4):
                rows = pl.ds(16 * i, 16)
                copies.append(pltpu.make_async_copy(ref.at[l, rows], hbm.at[l, rows], sem.at[len(copies)]))
    for cp in copies:
        cp.start()
    for cp in copies:
        cp.wait()


def fused(pos, x, vecs, w_qkv, w_out, w_in, w_down, k_cache, v_cache):
    specs, steps = make_plan()
    parts = len(specs)
    vmem = pl.BlockSpec(memory_space=pltpu.VMEM)
    hbm = pl.BlockSpec(memory_space=pl.ANY)
    lead = (4, 2, 2, 2)
    dma = pltpu.SemaphoreType.DMA
    outs = (x, k_cache, v_cache)
    y, k_new, v_new = pl.pallas_call(
        functools.partial(kernel, specs, steps),
        out_shape=tuple(pltpu.VMEM(a.shape, a.dtype) for a in outs),
        in_specs=[pl.BlockSpec(memory_space=pltpu.SMEM), vmem] + [vmem] * len(vecs) + [hbm] * 6,
        out_specs=[vmem] * 3,
        scratch_shapes=[
            pltpu.VMEM((1,) + lead + (VEC_ROWS, 128), F32),
            pltpu.VMEM((2,) + lead + (24, 3 * D), BF16),
            pltpu.VMEM((2,) + lead + (24, D), BF16),
            pltpu.VMEM((2,) + lead + (24, HID), BF16),
            pltpu.VMEM((2, 4, 2, 2, 96, D), BF16),
            pltpu.VMEM((ROWS, D), BF16),
            pltpu.VMEM((2, ROWS, D), BF16),
            pltpu.VMEM((2, ROWS, D), F32),
            pltpu.VMEM((2, ROWS, D), F32),
            pltpu.VMEM((ROWS, D), BF16),
            pltpu.VMEM((2 * ROWS, D), BF16),
            pltpu.VMEM((2 * ROWS, HID), BF16),
            pltpu.VMEM((ROWS, D), F32),
            pltpu.VMEM((9, ROWS, 128), F32),
            pltpu.VMEM((ROWS, 128), F32),
            pltpu.VMEM((VEC_ROWS, D), F32),
            pltpu.VMEM((2, 1, 3 * D), F32),
            pltpu.VMEM((2, 1, HID), F32),
            pltpu.VMEM((16 * ROWS, 128), F32),
            pltpu.VMEM((16 * ROWS, 128), F32),
            pltpu.VMEM((16 * ROWS, 128), F32),
            pltpu.VMEM((16 * ROWS, 128), F32),
            pltpu.VMEM((16 * SEQS, KEYS), F32),
            dma((16,)), dma((parts, SENDS)), dma((parts, SENDS)), dma((2,)), dma((2,)), dma((2, 2)), dma((2, 2)), dma((2, 2 * BLOCKS)),
        ],
        compiler_params=pltpu.CompilerParams(collective_id=0, has_side_effects=True, vmem_limit_bytes=VMEM_LIMIT),
    )(pos, x, *vecs, w_qkv, w_out, w_in, w_down, k_cache, v_cache)
    return pl.pallas_call(
        write_kernel,
        out_shape=tuple(jax.ShapeDtypeStruct(a.shape, a.dtype) for a in outs),
        in_specs=[vmem] * 3,
        out_specs=[hbm] * 3,
        scratch_shapes=[dma((17,))],
        compiler_params=pltpu.CompilerParams(vmem_limit_bytes=VMEM_SMALL),
    )(y, k_new, v_new)


def solution(mesh):
    row_spec = P('dp', None)
    vec_spec = P(None, 'dp')
    mat_spec = P(None, 'dp', None)
    cache_spec = P(None, 'dp', None, None, None)
    in_specs = (row_spec, P('dp'), cache_spec, cache_spec, vec_spec, vec_spec, vec_spec, vec_spec, mat_spec, vec_spec, mat_spec, vec_spec, mat_spec, vec_spec, mat_spec, vec_spec, P('dp'), P('dp'))
    out_specs = (row_spec, cache_spec, cache_spec)

    def device_step(x_embed, positions, k_cache, v_cache, ln1_gain, ln1_bias, ln2_gain, ln2_bias, w_qkv, b_qkv, w_out, b_out, w_in, b_in, w_down, b_down, lnf_gain, lnf_bias):
        vecs = (ln1_gain, ln1_bias, ln2_gain, ln2_bias, b_out, b_down, lnf_gain[None], lnf_bias[None], b_qkv, b_in)
        by_head = lambda a: jnp.swapaxes(a, 2, 3)
        out, k_new, v_new = fused(positions, x_embed, vecs, w_qkv, w_out, w_in, w_down, by_head(k_cache), by_head(v_cache))
        return out, by_head(k_new), by_head(v_new)

    return jax.shard_map(device_step, mesh=mesh, in_specs=in_specs, out_specs=out_specs, check_vma=False)
```

```python
import collections
import functools
import heapq
import itertools
import math
import jax
import jax.numpy as jnp
import numpy as np
from jax import lax
from jax.experimental import pallas as pl
from jax.experimental.pallas import tpu as pltpu
from jax.sharding import PartitionSpec as P

LN_EPS = 1e-5
ROPE_BASE = 10000.0
MESH = pl.DeviceIdType.MESH
F32, BF16 = jnp.float32, jnp.bfloat16
NZ = 4
Z, Y, X, C = 0, 1, 2, 3
Z1, Z2, Z3 = 4, 5, 6
ALONG_Z = (Z1, Z2, Z3)
DIMS = (4, 2, 2, 2)
VEC_ROWS = 24
ROWS, D, HEADS, HEAD, SLOTS, FF = 64, 768, 12, 64, 32, 3072
KEYS = HEADS * SLOTS
HID = FF // 2
SEQS = 8
BLOCKS = ROWS // SEQS
VMEM_LIMIT, VMEM_SMALL = 36 << 20, 1 << 20
FREQS = tuple(float(np.float32(1.0) / np.float32(ROPE_BASE) ** (np.float32(2 * i) / np.float32(16))) for i in range(8))
FIRST = 4
SENDS = 9


LINK, CORES = 46600.0, 300000.0
FIXED, FIXED_CORES = 1.6, 0.9
WINDOW, SLACK = 3, -1
ZXY, ZYX, XYZ, YXZ = ALONG_Z + (X, Y), ALONG_Z + (Y, X), (X, Y) + ALONG_Z, (Y, X) + ALONG_Z
YZX, ZX, XZ = (Y,) + ALONG_Z + (X,), ALONG_Z + (X,), (X,) + ALONG_Z
SHARES = {
    'vec': [((1, ZXY),)],
    'qkv': [((6, ZXY),), ((6, ZXY),)],
    'out': [((6, ZXY),), ((6, ZXY),)],
    'win': [((3, YZX),)] * 2,
    'down': [((2, ZX), (1, XZ))] * 2,
}
GROUPS = tuple((f, l, i) for f, layers, n in (('vec', 1, 1), ('qkv', 2, 3), ('win', 2, 4), ('down', 2, 2), ('out', 2, 1)) for l in range(layers) for i in range(n))
SEQUENCE = tuple(GROUPS[ord(k) - ord('a')] for k in 'tcbjakdligfhsequopmnr')


def group_parts(family, l, i):
    out, at = [], {'qkv': D, 'win': HID // 4, 'down': D // 2}.get(family, 0) * i
    for units, order in SHARES[family][l]:
        out.append((family, l, at, units * 128, order))
        at += units * 128
    return out


def gathered(order, phase):
    return {Z if d == Z3 else d for d in order[:phase]} - {Z1, Z2}


def sends(spec, phase, chip):
    family, _, _, width, order = spec
    size, z = width * {'vec': VEC_ROWS * 4, 'down': 192}.get(family, 48), chip[Z]
    for d in gathered(order, phase):
        size *= DIMS[d]
    if phase == len(order):
        return [(chip, size, chip)]
    axis = order[phase]
    if axis in ALONG_Z:
        hop, out = axis - Z1, []
        if hop <= z < NZ - 1:
            out.append(((z + 1,) + chip[1:], size, (Z, True) + chip))
        if 0 < z < NZ - hop:
            out.append(((z - 1,) + chip[1:], size, (Z, False) + chip))
        return out
    to = tuple(1 - v if e == axis else v for e, v in enumerate(chip))
    return [(to, size, (axis,) + chip)]


def comes(order, phase, chip):
    if phase == len(order) or order[phase] not in ALONG_Z:
        return 1
    hop = order[phase] - Z1
    return (chip[Z] > hop) + (chip[Z] + hop + 1 < NZ)


def arrivals(groups):
    chips = list(itertools.product(range(4), range(2), range(2)))
    free, heap, got, at, times = {}, [], collections.Counter(), collections.Counter(), collections.defaultdict(list)
    set_out, ticket = {chip: WINDOW for chip in chips}, itertools.count()

    def send(now, chip, g, i, phase):
        for to, size, link in sends(groups[g][i], phase, chip):
            own = to == chip
            free[link] = max(now, free.get(link, 0.0)) + size / (CORES if own else LINK)
            heapq.heappush(heap, (free[link] + (FIXED_CORES if own else FIXED), next(ticket), to, g, i, phase))

    for chip in chips:
        for g in range(WINDOW):
            for i in range(len(groups[g])):
                send(0.0, chip, g, i, 0)
    while heap:
        now, _, chip, g, i, phase = heapq.heappop(heap)
        got[chip, g, i, phase] += 1
        order = groups[g][i][4]
        while at[chip, g, i] <= len(order) and got[chip, g, i, at[chip, g, i]] == comes(order, at[chip, g, i], chip):
            over = at[chip, g, i]
            times[g, i, over].append(now)
            at[chip, g, i] += 1
            if over < len(order):
                send(now, chip, g, i, over + 1)
            if over == 0:
                got[chip, g] += 1
                if got[chip, g] == len(groups[g]) and set_out[chip] < len(groups):
                    later = set_out[chip]
                    set_out[chip] += 1
                    for j in range(len(groups[later])):
                        send(now, chip, later, j, 0)
    mean = {k: sum(v) / len(v) for k, v in times.items()}
    for g, i, phase in sorted(mean):
        if phase:
            mean[g, i, phase] = max(mean[g, i, phase], mean[g, i, phase - 1])
    return sorted((v, k) for k, v in mean.items())


def compute_tasks():
    out = {'vec': ([('vec', 0, 0)], [], 1.1)}
    for l in range(2):
        out[f's{l}'] = ([], ['o0'] if l else ['vec'], 0.25)
        for i in range(3):
            out[f'q{l}{i}'] = ([('qkv', l, i)], [f's{l}'], 0.4)
        out[f'h{l}'] = ([], [f's{l}'], 0.4)
        for i in range(4):
            out[f'w{l}{i}'] = ([('win', l, i)], [f'h{l}'], 0.3)
        for i in range(2):
            out[f'd{l}{i}'] = ([('down', l, i)], [f'w{l}{k}' for k in range(4)], 0.4)
        for i in range(BLOCKS):
            out[f'a{l}{i}'] = ([], [f'q{l}{k}' for k in range(3)], 0.7)
        out[f'o{l}'] = ([('out', l, 0)], [f'a{l}{k}' for k in range(BLOCKS)] + [f'd{l}0', f'd{l}1'], 0.6)
    return out


def make_plan():
    groups = [group_parts(*name) for name in SEQUENCE]
    specs = [spec for group in groups for spec in group]
    index = {(g, i): sum(len(h) for h in groups[:g]) + i for g, group in enumerate(groups) for i in range(len(group))}
    events, tasks = arrivals(groups), compute_tasks()
    steps = [(index[g, i], -1) for g in range(WINDOW) for i in range(len(groups[g]))]
    done, left, first_left, set_out, clock = set(), collections.Counter(), collections.Counter(), WINDOW, 0.0
    for g, group in enumerate(groups):
        left[g] = sum(len(spec[4]) + 1 for spec in group)
        first_left[g] = len(group)
    for n, (when, (g, i, phase)) in enumerate(events):
        clock = max(clock, when)
        steps.append((index[g, i], phase))
        left[g] -= 1
        if left[g] == 0:
            done.add(SEQUENCE[g])
        if phase == 0:
            first_left[g] -= 1
            if first_left[g] == 0 and set_out < len(groups):
                steps += [(index[set_out, j], -1) for j in range(len(groups[set_out]))]
                set_out += 1
        until = events[n + 1][0] + SLACK if n + 1 < len(events) else math.inf
        while clock < until:
            ready = [k for k, (needs, after, _) in tasks.items() if done.issuperset(needs) and done.issuperset(after)]
            if not ready:
                break
            steps.append(ready[0])
            done.add(ready[0])
            clock += tasks.pop(ready[0])[2]
    assert not tasks
    return specs, steps


class Part:
    def __init__(self, ref, lead, cols, order, where, sems, held=(Z, Y, X), first=None):
        self.ref, self.lead, self.cols, self.order, self.where = ref, lead, cols, order, where
        self.send_sems, self.recv_sems, self.index = sems
        self.held, self.first = held, first

    def copy(self, phase, axis, to, slot, z):
        full = gathered(self.order, phase)
        if self.first is not None and phase > 0:
            full.add(Y)
        at = (z,) + self.where[1:]
        sel = tuple(pl.ds(0, DIMS[d]) if d in full else at[d] for d in self.held)
        blk = self.ref.at[self.lead + sel + (self.where[C], slice(None), self.cols)]
        w = list(self.where)
        w[axis] = to
        return pltpu.make_async_remote_copy(
            src_ref=self.first if phase == 0 and self.first is not None else blk, dst_ref=blk,
            send_sem=self.send_sems.at[self.index, slot], recv_sem=self.recv_sems.at[self.index, slot],
            device_id=((((w[0] * 2 + w[1]) * 2 + w[2]) * 2 + w[3]),), device_id_type=MESH)

    def copies(self, phase, mine):
        axis, z = self.order[phase] if phase < len(self.order) else C, self.where[Z]
        if axis not in ALONG_Z:
            return [(None, self.copy(phase, axis, 1 - self.where[axis], {X: 6, Y: 7, C: 8}[axis], z))]
        hop = axis - Z1
        if mine:
            return [((z >= hop) & (z < NZ - 1), self.copy(phase, Z, z + 1, hop, z - hop)),
                    ((z + hop < NZ) & (z > 0), self.copy(phase, Z, z - 1, 3 + hop, z + hop))]
        return [(z > hop, self.copy(phase, Z, z, hop, z - hop - 1)), (z + hop + 1 < NZ, self.copy(phase, Z, z, 3 + hop, z + hop + 1))]

    @property
    def phases(self):
        return len(self.order) + 1

    def each(self, phase, mine, act):
        for condition, cp in self.copies(phase, mine):
            if condition is None:
                act(cp)
            else:
                pl.when(condition)(functools.partial(act, cp))

    def start(self, phase):
        self.each(phase, True, lambda cp: cp.start())

    def finish(self, phase):
        self.each(phase, False, lambda cp: cp.wait_recv())

    def drain(self):
        for phase in range(self.phases):
            self.each(phase, True, lambda cp: cp.wait_send())


def iota(shape, axis):
    return lax.broadcasted_iota(jnp.int32, shape, axis)


def floor_div(values, width):
    return jnp.floor((values + 0.5) * (1.0 / width))


def dot(a, b):
    return jnp.dot(a, b, preferred_element_type=F32)


def layer_norm(x_f32, gain, bias):
    row_mean = jnp.mean(x_f32, axis=-1, keepdims=True)
    centered = x_f32 - row_mean
    row_var = jnp.mean(centered * centered, axis=-1, keepdims=True)
    return (centered * lax.rsqrt(row_var + LN_EPS) * gain + bias).astype(BF16)


def one_hot_cols(width, cols_f32):
    index = cols_f32 - floor_div(cols_f32, width) * width
    return (iota(index.shape, 0).astype(F32) == index).astype(BF16)


def kernel(specs, steps, pos_ref, x_ref, g1_ref, c1_ref, g2_ref, c2_ref, bo_ref, bd_ref, gf_ref, cf_ref, bq_ref, bi_ref, qkv_ref, out_ref, win_ref, down_ref, k_hbm, v_hbm,
           y_ref, kbuf, vbuf,
           vec_g, qkv_g, out_g, win_g, down_g, x1_scr, xn_scr, ps_scr, pr_scr, h1_scr, h2_scr, act_scr, acc_scr,
           rope_ref, pos_scr, vrow_scr, bq_scr, bi_scr, q_scr, kn_scr, vn_scr, ctx_scr, s_scr,
           own_sem, send_sems, recv_sems, xs_sem, xr_sem, ps_sem, pr_sem, in_sem):
    me = lax.axis_index('dp')
    where = (me // 8, (me // 4) % 2, (me // 2) % 2, me % 2)
    z, y, x, c = where

    def device(z, y, x, c):
        return (((z * 2 + y) * 2 + x) * 2 + c,)

    y_peer = device(z, 1 - y, x, c)

    def cache_in(i):
        l, rows = i // BLOCKS, pl.ds(i % BLOCKS * SEQS, SEQS)
        return [pltpu.make_async_copy(k_hbm.at[l, rows], kbuf.at[l, rows], in_sem.at[0, i]),
                pltpu.make_async_copy(v_hbm.at[l, rows], vbuf.at[l, rows], in_sem.at[1, i])]

    def my_cols(zb, yy):
        return pl.ds(pl.multiple_of(768 * zb + 384 * yy, 128), 384)

    own = [(qkv_ref.at[0], qkv_g.at[0, z, y, x, c])]
    own += [(win_ref.at[0, :, my_cols(zb, y)], win_g.at[0, z, y, x, c, :, pl.ds(384 * zb, 384)]) for zb in range(4)]
    own += [(down_ref.at[0], down_g.at[0, z, x, c]), (out_ref.at[0], out_g.at[0, z, y, x, c]), (qkv_ref.at[1], qkv_g.at[1, z, y, x, c])]
    own += [(win_ref.at[1, :, my_cols(zb, y)], win_g.at[1, z, y, x, c, :, pl.ds(384 * zb, 384)]) for zb in range(4)]
    own += [(down_ref.at[1], down_g.at[1, z, x, c]), (out_ref.at[1], out_g.at[1, z, y, x, c])]
    own = [pltpu.make_async_copy(src, dst, own_sem.at[i]) for i, (src, dst) in enumerate(own)]
    for cp in own:
        cp.start()

    barrier = pltpu.get_barrier_semaphore()
    for who in (device(z, y, 1 - x, c), y_peer, device(z, y, x, 1 - c)):
        pl.semaphore_signal(barrier, inc=1, device_id=who, device_id_type=MESH)
    for there, step in ((z > 0, -1), (z < NZ - 1, 1)):
        @pl.when(there)
        def _(step=step):
            pl.semaphore_signal(barrier, inc=1, device_id=device(z + step, y, x, c), device_id_type=MESH)
    own_vec = vec_g.at[0, z, y, x, c]
    own_vec[...] = jnp.zeros((VEC_ROWS, 128), F32)
    at_row = 0
    for ref in (g1_ref, c1_ref, g2_ref, c2_ref, bo_ref, bd_ref, gf_ref, cf_ref, bq_ref, bi_ref):
        count, width = ref.shape
        own_vec[pl.ds(at_row, count), pl.ds(0, width)] = ref[...].astype(F32)
        at_row += count

    pl.semaphore_wait(barrier, 3 + (z + 3) // 4 + (6 - z) // 4)
    for cp in own:
        cp.wait()
    refs = {'vec': vec_g, 'qkv': qkv_g, 'win': win_g, 'down': down_g, 'out': out_g}
    parts = []
    for i, (family, l, col, width, order) in enumerate(specs):
        kw = {}
        if family == 'down':
            kw['held'] = (Z, X)
        if family == 'win':
            kw['first'] = win_ref.at[l, :, pl.ds(pl.multiple_of(768 * (col // 384) + 384 * (1 - y) + col % 384, 128), width)]
        parts.append(Part(refs[family], (l,), pl.ds(col, width), order, where, (send_sems, recv_sems, i), **kw))

    lane = iota((1, 128), 1)

    def send_x(l):
        src = x_ref if l == 0 else x1_scr
        return pltpu.make_async_remote_copy(src_ref=src, dst_ref=xn_scr.at[l], send_sem=xs_sem.at[l], recv_sem=xr_sem.at[l],
                                            device_id=y_peer, device_id_type=MESH)

    def send_part(l, i):
        cols = pl.ds(384 * i, 384)
        return pltpu.make_async_remote_copy(src_ref=ps_scr.at[l, :, cols], dst_ref=pr_scr.at[l, :, cols], send_sem=ps_sem.at[l, i],
                                            recv_sem=pr_sem.at[l, i], device_id=y_peer, device_id_type=MESH)

    def task_rope():
        for b in range(ROWS):
            pos_scr[pl.ds(b, 1), :] = jnp.full((1, 128), pos_ref[b], jnp.int32).astype(F32)
        d = lane % HEAD
        freq = jnp.zeros((1, 128), F32)
        for i, f in enumerate(FREQS):
            freq = jnp.where(d % 8 == i, f, freq)
        angle = pos_scr[...] * freq
        cos, sin = jnp.cos(angle), jnp.sin(angle)
        for t, turned in enumerate((lane >= 0, lane >= 64, lane < 64)):
            rope_ref[3 * t] = jnp.where(turned & (d < 16), cos, 1.0)
            rope_ref[3 * t + 1] = jnp.where(turned & (d < 8), -sin, 0.0)
            rope_ref[3 * t + 2] = jnp.where(turned & (d >= 8) & (d < 16), sin, 0.0)

    def task_vec():
        vec2 = vec_g[...].reshape(32 * VEC_ROWS, 128).astype(BF16)
        n = iota((1, D), 1).astype(F32)
        spread = dot(vec2, one_hot_cols(24, jnp.broadcast_to(n, (128, D))))
        r = iota((32 * VEC_ROWS, 1), 0).astype(F32)
        mine = floor_div(n, 24) == floor_div(r, VEC_ROWS)
        spread = jnp.where(mine, spread, 0.0).astype(BF16)
        rr = iota((1, 32 * VEC_ROWS), 1).astype(F32)
        kind = rr - floor_div(rr, VEC_ROWS) * VEC_ROWS
        pick = (iota((VEC_ROWS, 32 * VEC_ROWS), 0).astype(F32) == kind).astype(BF16)
        vrow_scr[...] = dot(pick, spread)
        dev = iota((32, 1), 0).astype(F32)

        def long_row(kind, width, cols):
            g = vec_g[0, :, :, :, :, kind].reshape(32, 128).astype(BF16)
            n = cols.astype(F32)
            full = dot(g, one_hot_cols(width, jnp.broadcast_to(n, (128, n.shape[1]))))
            return jnp.sum(jnp.where(floor_div(n, width) == dev, full, 0.0), axis=0, keepdims=True)

        for l in range(2):
            bq_scr[l] = long_row(14 + l, 72, iota((1, 3 * D), 1))
            for zb in range(4):
                bi_scr[l, :, pl.ds(384 * zb, 384)] = long_row(16 + l, 96, iota((1, 384), 1) + (768 * zb + 384 * y))

    def vrow(kind):
        return vrow_scr[pl.ds(kind, 1), :]

    def x_of(l):
        return (x_ref if l == 0 else x1_scr)[...]

    def task_start(l):
        send_x(l).start()
        h1_scr[...] = layer_norm(x_of(l).astype(F32), vrow(l), vrow(2 + l))

    def task_qkv(l, i):
        w = qkv_g[l, :, :, :, :, :, pl.ds(768 * i, 768)].reshape(D, 768)
        got = (dot(h1_scr[...], w) + bq_scr[l, :, pl.ds(768 * i, 768)]).astype(BF16).astype(F32)
        for m in range(2):
            tiles = []
            for t in range(3):
                v = got[:, 384 * m + 128 * t: 384 * m + 128 * t + 128]
                r = v * rope_ref[3 * t] + pltpu.roll(v, 120, 1) * rope_ref[3 * t + 1] + pltpu.roll(v, 8, 1) * rope_ref[3 * t + 2]
                tiles.append(r.astype(BF16).astype(F32))
            h = 4 * i + 2 * m
            t0, t1, t2 = tiles
            q_scr[pl.ds(h, ROWS, stride=16), :] = t0
            kn_scr[pl.ds(h, ROWS, stride=16), :] = pltpu.roll(t0, 64, 1)
            vn_scr[pl.ds(h, ROWS, stride=16), :] = t1
            q_scr[pl.ds(h + 1, ROWS, stride=16), :] = pltpu.roll(t1, 64, 1)
            kn_scr[pl.ds(h + 1, ROWS, stride=16), :] = t2
            vn_scr[pl.ds(h + 1, ROWS, stride=16), :] = pltpu.roll(t2, 64, 1)

    def task_att(l, blk):
        for cp in cache_in(l * BLOCKS + blk):
            cp.wait()
        key = iota((1, KEYS), 1)
        head_row = jnp.minimum(iota((16, 1), 0), HEADS - 1) * SLOTS
        slot_of = key - head_row
        own_head = (slot_of >= 0) & (slot_of < SLOTS)
        slots = iota((SLOTS, HEAD), 0)

        def scores(j):
            b = blk * SEQS + j
            pos = pos_ref[b]
            rows = pl.ds(b * 16, 16)
            put = jnp.where(slots == pos, 1.0, 0.0).astype(BF16) > 0.5

            def placed(buf, new_scr):
                new = new_scr[rows, :][:HEADS, :HEAD].astype(BF16)
                both = jnp.where(put[None], new[:, None, :], buf[l, blk * SEQS + j])
                buf[l, blk * SEQS + j] = both
                return both.reshape(KEYS, HEAD)

            keys = placed(kbuf, kn_scr)
            placed(vbuf, vn_scr)
            q = q_scr[rows, :][:, :HEAD].astype(BF16)
            s = lax.dot_general(q, keys, (((1,), (1,)), ((), ())), preferred_element_type=F32) * (HEAD ** -0.5)
            s_scr[pl.ds(j * 16, 16), :] = jnp.where(own_head & (slot_of <= pos), s, -jnp.inf)

        def weighted(j):
            p = s_scr[pl.ds(j * 16, 16), :].astype(BF16)
            got = dot(p, vbuf[l, blk * SEQS + j].reshape(KEYS, HEAD))
            ctx_scr[pl.ds((blk * SEQS + j) * 16, 16), pl.ds(0, HEAD)] = got

        for j in range(SEQS):
            scores(j)
        s = s_scr[...]
        e = jnp.exp(s - jnp.max(s, axis=-1, keepdims=True))
        s_scr[...] = e / jnp.sum(e, axis=-1, keepdims=True)
        for j in range(SEQS):
            weighted(j)

    def task_h2(l):
        send_x(l).wait_recv()
        for half, v in enumerate((x_of(l), xn_scr[l])):
            h2_scr[pl.ds(ROWS * half, ROWS), :] = layer_norm(v.astype(F32), vrow(4 + l), vrow(6 + l))

    def task_win(l, zb):
        cols = pl.ds(384 * zb, 384)
        w = win_g[l, :, :, :, :, :, cols].reshape(D, 384)
        u = dot(h2_scr[...], w) + bi_scr[l, :, cols]
        act_scr[:, cols] = (0.5 * u * (1.0 + lax.erf(u * 0.7071067811865476))).astype(BF16)

    def task_down(l, i):
        cols = pl.ds(384 * i, 384)
        got = dot(act_scr[...], down_g[l, :, :, :, :, cols].reshape(HID, 384))
        acc_scr[:, cols] = got[:ROWS]
        ps_scr[l, :, cols] = got[ROWS:]
        send_part(l, i).start()

    def task_out(l):
        tiles = []
        for m in range(HEADS // 2):
            a = ctx_scr[pl.ds(2 * m, ROWS, stride=16), :]
            b = pltpu.roll(ctx_scr[pl.ds(2 * m + 1, ROWS, stride=16), :], 64, 1)
            tiles.append(jnp.where(lane < 64, a, b).astype(BF16))
        a = dot(jnp.concatenate(tiles, axis=1), out_g[l].reshape(D, D)) + vrow(8 + l)
        for i in range(2):
            send_part(l, i).wait_recv()
        m = acc_scr[...] + pr_scr[l] + vrow(10 + l)
        new = (x_of(l).astype(F32) + a + m).astype(BF16)
        if l == 0:
            x1_scr[...] = new
        else:
            y_ref[...] = layer_norm(new.astype(F32), vrow(12), vrow(13))

    tasks = {'vec': task_vec}
    for l in range(2):
        tasks[f's{l}'] = functools.partial(task_start, l)
        tasks[f'h{l}'] = functools.partial(task_h2, l)
        tasks[f'o{l}'] = functools.partial(task_out, l)
        for name, fn, count in (('q', task_qkv, 3), ('w', task_win, 4), ('d', task_down, 2), ('a', task_att, BLOCKS)):
            for i in range(count):
                tasks[f'{name}{l}{i}'] = functools.partial(fn, l, i)

    for n, step in enumerate(steps):
        if isinstance(step, str):
            tasks.pop(step)()
            continue
        p, phase = parts[step[0]], step[1]
        if phase >= 0:
            p.finish(phase)
        if phase + 1 < p.phases:
            p.start(phase + 1)
        if n == FIRST:
            for i in range(2 * BLOCKS):
                for cp in cache_in(i):
                    cp.start()
            task_rope()
    assert not tasks

    for p in parts:
        p.drain()
    for l in range(2):
        send_x(l).wait_send()
        for i in range(2):
            send_part(l, i).wait_send()


def write_kernel(y_ref, k_ref, v_ref, y_hbm, k_hbm, v_hbm, sem):
    copies = [pltpu.make_async_copy(y_ref, y_hbm, sem.at[0])]
    for ref, hbm in ((k_ref, k_hbm), (v_ref, v_hbm)):
        for l in range(2):
            for i in range(4):
                rows = pl.ds(16 * i, 16)
                copies.append(pltpu.make_async_copy(ref.at[l, rows], hbm.at[l, rows], sem.at[len(copies)]))
    for cp in copies:
        cp.start()
    for cp in copies:
        cp.wait()


def fused(pos, x, vecs, w_qkv, w_out, w_in, w_down, k_cache, v_cache):
    specs, steps = make_plan()
    parts = len(specs)
    vmem = pl.BlockSpec(memory_space=pltpu.VMEM)
    hbm = pl.BlockSpec(memory_space=pl.ANY)
    lead = (4, 2, 2, 2)
    dma = pltpu.SemaphoreType.DMA
    outs = (x, k_cache, v_cache)
    y, k_new, v_new = pl.pallas_call(
        functools.partial(kernel, specs, steps),
        out_shape=tuple(pltpu.VMEM(a.shape, a.dtype) for a in outs),
        in_specs=[pl.BlockSpec(memory_space=pltpu.SMEM), vmem] + [vmem] * len(vecs) + [hbm] * 6,
        out_specs=[vmem] * 3,
        scratch_shapes=[
            pltpu.VMEM((1,) + lead + (VEC_ROWS, 128), F32),
            pltpu.VMEM((2,) + lead + (24, 3 * D), BF16),
            pltpu.VMEM((2,) + lead + (24, D), BF16),
            pltpu.VMEM((2,) + lead + (24, HID), BF16),
            pltpu.VMEM((2, 4, 2, 2, 96, D), BF16),
            pltpu.VMEM((ROWS, D), BF16),
            pltpu.VMEM((2, ROWS, D), BF16),
            pltpu.VMEM((2, ROWS, D), F32),
            pltpu.VMEM((2, ROWS, D), F32),
            pltpu.VMEM((ROWS, D), BF16),
            pltpu.VMEM((2 * ROWS, D), BF16),
            pltpu.VMEM((2 * ROWS, HID), BF16),
            pltpu.VMEM((ROWS, D), F32),
            pltpu.VMEM((9, ROWS, 128), F32),
            pltpu.VMEM((ROWS, 128), F32),
            pltpu.VMEM((VEC_ROWS, D), F32),
            pltpu.VMEM((2, 1, 3 * D), F32),
            pltpu.VMEM((2, 1, HID), F32),
            pltpu.VMEM((16 * ROWS, 128), F32),
            pltpu.VMEM((16 * ROWS, 128), F32),
            pltpu.VMEM((16 * ROWS, 128), F32),
            pltpu.VMEM((16 * ROWS, 128), F32),
            pltpu.VMEM((16 * SEQS, KEYS), F32),
            dma((16,)), dma((parts, SENDS)), dma((parts, SENDS)), dma((2,)), dma((2,)), dma((2, 2)), dma((2, 2)), dma((2, 2 * BLOCKS)),
        ],
        compiler_params=pltpu.CompilerParams(collective_id=0, has_side_effects=True, vmem_limit_bytes=VMEM_LIMIT),
    )(pos, x, *vecs, w_qkv, w_out, w_in, w_down, k_cache, v_cache)
    return pl.pallas_call(
        write_kernel,
        out_shape=tuple(jax.ShapeDtypeStruct(a.shape, a.dtype) for a in outs),
        in_specs=[vmem] * 3,
        out_specs=[hbm] * 3,
        scratch_shapes=[dma((17,))],
        compiler_params=pltpu.CompilerParams(vmem_limit_bytes=VMEM_SMALL),
    )(y, k_new, v_new)


def solution(mesh):
    row_spec = P('dp', None)
    vec_spec = P(None, 'dp')
    mat_spec = P(None, 'dp', None)
    cache_spec = P(None, 'dp', None, None, None)
    in_specs = (row_spec, P('dp'), cache_spec, cache_spec, vec_spec, vec_spec, vec_spec, vec_spec, mat_spec, vec_spec, mat_spec, vec_spec, mat_spec, vec_spec, mat_spec, vec_spec, P('dp'), P('dp'))
    out_specs = (row_spec, cache_spec, cache_spec)

    def device_step(x_embed, positions, k_cache, v_cache, ln1_gain, ln1_bias, ln2_gain, ln2_bias, w_qkv, b_qkv, w_out, b_out, w_in, b_in, w_down, b_down, lnf_gain, lnf_bias):
        vecs = (ln1_gain, ln1_bias, ln2_gain, ln2_bias, b_out, b_down, lnf_gain[None], lnf_bias[None], b_qkv, b_in)
        by_head = lambda a: jnp.swapaxes(a, 2, 3)
        out, k_new, v_new = fused(positions, x_embed, vecs, w_qkv, w_out, w_in, w_down, by_head(k_cache), by_head(v_cache))
        return out, by_head(k_new), by_head(v_new)

    return jax.shard_map(device_step, mesh=mesh, in_specs=in_specs, out_specs=out_specs, check_vma=False)
```

```python
import collections
import functools
import heapq
import itertools
import math
import jax
import jax.numpy as jnp
import numpy as np
from jax import lax
from jax.experimental import pallas as pl
from jax.experimental.pallas import tpu as pltpu
from jax.sharding import PartitionSpec as P

LN_EPS = 1e-5
ROPE_BASE = 10000.0
MESH = pl.DeviceIdType.MESH
F32, BF16 = jnp.float32, jnp.bfloat16
NZ = 4
Z, Y, X, C = 0, 1, 2, 3
Z1, Z2, Z3 = 4, 5, 6
ALONG_Z = (Z1, Z2, Z3)
DIMS = (4, 2, 2, 2)
VEC_ROWS = 24
ROWS, D, HEADS, HEAD, SLOTS, FF = 64, 768, 12, 64, 32, 3072
KEYS = HEADS * SLOTS
HID = FF // 2
SEQS = 8
BLOCKS = ROWS // SEQS
VMEM_LIMIT, VMEM_SMALL = 36 << 20, 1 << 20
FREQS = tuple(float(np.float32(1.0) / np.float32(ROPE_BASE) ** (np.float32(2 * i) / np.float32(16))) for i in range(8))
FIRST = 4
SENDS = 9


LINK, CORES = 46600.0, 300000.0
FIXED, FIXED_CORES = 1.6, 0.9
WINDOW, SLACK = 3, -1
ZXY, ZYX, XYZ, YXZ = ALONG_Z + (X, Y), ALONG_Z + (Y, X), (X, Y) + ALONG_Z, (Y, X) + ALONG_Z
YZX, ZX, XZ = (Y,) + ALONG_Z + (X,), ALONG_Z + (X,), (X,) + ALONG_Z
SHARES = {
    'vec': [((1, ZXY),)],
    'qkv': [((5, ZXY), (1, YXZ)), ((6, ZXY),)],
    'out': [((6, ZXY),), ((6, ZXY),)],
    'win': [((3, YZX),)] * 2,
    'down': [((2, ZX), (1, XZ))] * 2,
}
GROUPS = tuple((f, l, i) for f, layers, n in (('vec', 1, 1), ('qkv', 2, 3), ('win', 2, 4), ('down', 2, 2), ('out', 2, 1)) for l in range(layers) for i in range(n))
SEQUENCE = tuple(GROUPS[ord(k) - ord('a')] for k in 'acfktgjibodephulqsnrm')


def group_parts(family, l, i):
    out, at = [], {'qkv': D, 'win': HID // 4, 'down': D // 2}.get(family, 0) * i
    for units, order in SHARES[family][l]:
        out.append((family, l, at, units * 128, order))
        at += units * 128
    return out


def gathered(order, phase):
    return {Z if d == Z3 else d for d in order[:phase]} - {Z1, Z2}


def sends(spec, phase, chip):
    family, _, _, width, order = spec
    size, z = width * {'vec': VEC_ROWS * 4, 'down': 192}.get(family, 48), chip[Z]
    for d in gathered(order, phase):
        size *= DIMS[d]
    if phase == len(order):
        return [(chip, size, chip)]
    axis = order[phase]
    if axis in ALONG_Z:
        hop, out = axis - Z1, []
        if hop <= z < NZ - 1:
            out.append(((z + 1,) + chip[1:], size, (Z, True) + chip))
        if 0 < z < NZ - hop:
            out.append(((z - 1,) + chip[1:], size, (Z, False) + chip))
        return out
    to = tuple(1 - v if e == axis else v for e, v in enumerate(chip))
    return [(to, size, (axis,) + chip)]


def comes(order, phase, chip):
    if phase == len(order) or order[phase] not in ALONG_Z:
        return 1
    hop = order[phase] - Z1
    return (chip[Z] > hop) + (chip[Z] + hop + 1 < NZ)


def arrivals(groups):
    chips = list(itertools.product(range(4), range(2), range(2)))
    free, heap, got, at, times = {}, [], collections.Counter(), collections.Counter(), collections.defaultdict(list)
    set_out, ticket = {chip: WINDOW for chip in chips}, itertools.count()

    def send(now, chip, g, i, phase):
        for to, size, link in sends(groups[g][i], phase, chip):
            own = to == chip
            free[link] = max(now, free.get(link, 0.0)) + size / (CORES if own else LINK)
            heapq.heappush(heap, (free[link] + (FIXED_CORES if own else FIXED), next(ticket), to, g, i, phase))

    for chip in chips:
        for g in range(WINDOW):
            for i in range(len(groups[g])):
                send(0.0, chip, g, i, 0)
    while heap:
        now, _, chip, g, i, phase = heapq.heappop(heap)
        got[chip, g, i, phase] += 1
        order = groups[g][i][4]
        while at[chip, g, i] <= len(order) and got[chip, g, i, at[chip, g, i]] == comes(order, at[chip, g, i], chip):
            over = at[chip, g, i]
            times[g, i, over].append(now)
            at[chip, g, i] += 1
            if over < len(order):
                send(now, chip, g, i, over + 1)
            if over == 0:
                got[chip, g] += 1
                if got[chip, g] == len(groups[g]) and set_out[chip] < len(groups):
                    later = set_out[chip]
                    set_out[chip] += 1
                    for j in range(len(groups[later])):
                        send(now, chip, later, j, 0)
    mean = {k: sum(v) / len(v) for k, v in times.items()}
    for g, i, phase in sorted(mean):
        if phase:
            mean[g, i, phase] = max(mean[g, i, phase], mean[g, i, phase - 1])
    return sorted((v, k) for k, v in mean.items())


def compute_tasks():
    out = {'vec': ([('vec', 0, 0)], [], 1.1)}
    for l in range(2):
        out[f's{l}'] = ([], ['o0'] if l else ['vec'], 0.25)
        for i in range(3):
            out[f'q{l}{i}'] = ([('qkv', l, i)], [f's{l}'], 0.4)
        out[f'h{l}'] = ([], [f's{l}'], 0.4)
        for i in range(4):
            out[f'w{l}{i}'] = ([('win', l, i)], [f'h{l}'], 0.3)
        for i in range(2):
            out[f'd{l}{i}'] = ([('down', l, i)], [f'w{l}{k}' for k in range(4)], 0.4)
        for i in range(BLOCKS):
            out[f'a{l}{i}'] = ([], [f'q{l}{k}' for k in range(3)], 0.7)
        out[f'o{l}'] = ([('out', l, 0)], [f'a{l}{k}' for k in range(BLOCKS)] + [f'd{l}0', f'd{l}1'], 0.6)
    return out


def make_plan():
    groups = [group_parts(*name) for name in SEQUENCE]
    specs = [spec for group in groups for spec in group]
    index = {(g, i): sum(len(h) for h in groups[:g]) + i for g, group in enumerate(groups) for i in range(len(group))}
    events, tasks = arrivals(groups), compute_tasks()
    steps = [(index[g, i], -1) for g in range(WINDOW) for i in range(len(groups[g]))]
    done, left, first_left, set_out, clock = set(), collections.Counter(), collections.Counter(), WINDOW, 0.0
    for g, group in enumerate(groups):
        left[g] = sum(len(spec[4]) + 1 for spec in group)
        first_left[g] = len(group)
    for n, (when, (g, i, phase)) in enumerate(events):
        clock = max(clock, when)
        steps.append((index[g, i], phase))
        left[g] -= 1
        if left[g] == 0:
            done.add(SEQUENCE[g])
        if phase == 0:
            first_left[g] -= 1
            if first_left[g] == 0 and set_out < len(groups):
                steps += [(index[set_out, j], -1) for j in range(len(groups[set_out]))]
                set_out += 1
        until = events[n + 1][0] + SLACK if n + 1 < len(events) else math.inf
        while clock < until:
            ready = [k for k, (needs, after, _) in tasks.items() if done.issuperset(needs) and done.issuperset(after)]
            if not ready:
                break
            steps.append(ready[0])
            done.add(ready[0])
            clock += tasks.pop(ready[0])[2]
    assert not tasks
    return specs, steps


class Part:
    def __init__(self, ref, lead, cols, order, where, sems, held=(Z, Y, X), first=None):
        self.ref, self.lead, self.cols, self.order, self.where = ref, lead, cols, order, where
        self.send_sems, self.recv_sems, self.index = sems
        self.held, self.first = held, first

    def copy(self, phase, axis, to, slot, z):
        full = gathered(self.order, phase)
        if self.first is not None and phase > 0:
            full.add(Y)
        at = (z,) + self.where[1:]
        sel = tuple(pl.ds(0, DIMS[d]) if d in full else at[d] for d in self.held)
        blk = self.ref.at[self.lead + sel + (self.where[C], slice(None), self.cols)]
        w = list(self.where)
        w[axis] = to
        return pltpu.make_async_remote_copy(
            src_ref=self.first if phase == 0 and self.first is not None else blk, dst_ref=blk,
            send_sem=self.send_sems.at[self.index, slot], recv_sem=self.recv_sems.at[self.index, slot],
            device_id=((((w[0] * 2 + w[1]) * 2 + w[2]) * 2 + w[3]),), device_id_type=MESH)

    def copies(self, phase, mine):
        axis, z = self.order[phase] if phase < len(self.order) else C, self.where[Z]
        if axis not in ALONG_Z:
            return [(None, self.copy(phase, axis, 1 - self.where[axis], {X: 6, Y: 7, C: 8}[axis], z))]
        hop = axis - Z1
        if mine:
            return [((z >= hop) & (z < NZ - 1), self.copy(phase, Z, z + 1, hop, z - hop)),
                    ((z + hop < NZ) & (z > 0), self.copy(phase, Z, z - 1, 3 + hop, z + hop))]
        return [(z > hop, self.copy(phase, Z, z, hop, z - hop - 1)), (z + hop + 1 < NZ, self.copy(phase, Z, z, 3 + hop, z + hop + 1))]

    @property
    def phases(self):
        return len(self.order) + 1

    def each(self, phase, mine, act):
        for condition, cp in self.copies(phase, mine):
            if condition is None:
                act(cp)
            else:
                pl.when(condition)(functools.partial(act, cp))

    def start(self, phase):
        self.each(phase, True, lambda cp: cp.start())

    def finish(self, phase):
        self.each(phase, False, lambda cp: cp.wait_recv())

    def drain(self):
        for phase in range(self.phases):
            self.each(phase, True, lambda cp: cp.wait_send())


def iota(shape, axis):
    return lax.broadcasted_iota(jnp.int32, shape, axis)


def floor_div(values, width):
    return jnp.floor((values + 0.5) * (1.0 / width))


def dot(a, b):
    return jnp.dot(a, b, preferred_element_type=F32)


def layer_norm(x_f32, gain, bias):
    row_mean = jnp.mean(x_f32, axis=-1, keepdims=True)
    centered = x_f32 - row_mean
    row_var = jnp.mean(centered * centered, axis=-1, keepdims=True)
    return (centered * lax.rsqrt(row_var + LN_EPS) * gain + bias).astype(BF16)


def one_hot_cols(width, cols_f32):
    index = cols_f32 - floor_div(cols_f32, width) * width
    return (iota(index.shape, 0).astype(F32) == index).astype(BF16)


def kernel(specs, steps, pos_ref, x_ref, g1_ref, c1_ref, g2_ref, c2_ref, bo_ref, bd_ref, gf_ref, cf_ref, bq_ref, bi_ref, qkv_ref, out_ref, win_ref, down_ref, k_hbm, v_hbm,
           y_ref, kbuf, vbuf,
           vec_g, qkv_g, out_g, win_g, down_g, x1_scr, xn_scr, ps_scr, pr_scr, h1_scr, h2_scr, act_scr, acc_scr,
           rope_ref, pos_scr, vrow_scr, bq_scr, bi_scr, q_scr, kn_scr, vn_scr, ctx_scr, s_scr,
           own_sem, send_sems, recv_sems, xs_sem, xr_sem, ps_sem, pr_sem, in_sem):
    me = lax.axis_index('dp')
    where = (me // 8, (me // 4) % 2, (me // 2) % 2, me % 2)
    z, y, x, c = where

    def device(z, y, x, c):
        return (((z * 2 + y) * 2 + x) * 2 + c,)

    y_peer = device(z, 1 - y, x, c)

    def cache_in(i):
        l, rows = i // BLOCKS, pl.ds(i % BLOCKS * SEQS, SEQS)
        return [pltpu.make_async_copy(k_hbm.at[l, rows], kbuf.at[l, rows], in_sem.at[0, i]),
                pltpu.make_async_copy(v_hbm.at[l, rows], vbuf.at[l, rows], in_sem.at[1, i])]

    def my_cols(zb, yy):
        return pl.ds(pl.multiple_of(768 * zb + 384 * yy, 128), 384)

    own = {'vec0': []}
    for l in range(2):
        own[f'qkv{l}'] = [(qkv_ref.at[l], qkv_g.at[l, z, y, x, c])]
        own[f'win{l}'] = [(win_ref.at[l, :, my_cols(zb, y)], win_g.at[l, z, y, x, c, :, pl.ds(384 * zb, 384)]) for zb in range(4)]
        own[f'down{l}'] = [(down_ref.at[l], down_g.at[l, z, x, c])]
        own[f'out{l}'] = [(out_ref.at[l], out_g.at[l, z, y, x, c])]
    count = itertools.count()
    own = {k: [pltpu.make_async_copy(src, dst, own_sem.at[next(count)]) for src, dst in v] for k, v in own.items()}
    for cp in itertools.chain(*own.values()):
        cp.start()

    barrier = pltpu.get_barrier_semaphore()
    for who in (device(z, y, 1 - x, c), y_peer, device(z, y, x, 1 - c)):
        pl.semaphore_signal(barrier, inc=1, device_id=who, device_id_type=MESH)
    for there, step in ((z > 0, -1), (z < NZ - 1, 1)):
        @pl.when(there)
        def _(step=step):
            pl.semaphore_signal(barrier, inc=1, device_id=device(z + step, y, x, c), device_id_type=MESH)
    own_vec = vec_g.at[0, z, y, x, c]
    own_vec[...] = jnp.zeros((VEC_ROWS, 128), F32)
    at_row = 0
    for ref in (g1_ref, c1_ref, g2_ref, c2_ref, bo_ref, bd_ref, gf_ref, cf_ref, bq_ref, bi_ref):
        count, width = ref.shape
        own_vec[pl.ds(at_row, count), pl.ds(0, width)] = ref[...].astype(F32)
        at_row += count

    pl.semaphore_wait(barrier, 3 + (z + 3) // 4 + (6 - z) // 4)
    refs = {'vec': vec_g, 'qkv': qkv_g, 'win': win_g, 'down': down_g, 'out': out_g}
    parts = []
    for i, (family, l, col, width, order) in enumerate(specs):
        kw = {}
        if family == 'down':
            kw['held'] = (Z, X)
        if family == 'win':
            kw['first'] = win_ref.at[l, :, pl.ds(pl.multiple_of(768 * (col // 384) + 384 * (1 - y) + col % 384, 128), width)]
        parts.append(Part(refs[family], (l,), pl.ds(col, width), order, where, (send_sems, recv_sems, i), **kw))

    lane = iota((1, 128), 1)

    def send_x(l):
        src = x_ref if l == 0 else x1_scr
        return pltpu.make_async_remote_copy(src_ref=src, dst_ref=xn_scr.at[l], send_sem=xs_sem.at[l], recv_sem=xr_sem.at[l],
                                            device_id=y_peer, device_id_type=MESH)

    def send_part(l, i):
        cols = pl.ds(384 * i, 384)
        return pltpu.make_async_remote_copy(src_ref=ps_scr.at[l, :, cols], dst_ref=pr_scr.at[l, :, cols], send_sem=ps_sem.at[l, i],
                                            recv_sem=pr_sem.at[l, i], device_id=y_peer, device_id_type=MESH)

    def task_rope():
        for b in range(ROWS):
            pos_scr[pl.ds(b, 1), :] = jnp.full((1, 128), pos_ref[b], jnp.int32).astype(F32)
        d = lane % HEAD
        freq = jnp.zeros((1, 128), F32)
        for i, f in enumerate(FREQS):
            freq = jnp.where(d % 8 == i, f, freq)
        angle = pos_scr[...] * freq
        cos, sin = jnp.cos(angle), jnp.sin(angle)
        for t, turned in enumerate((lane >= 0, lane >= 64, lane < 64)):
            rope_ref[3 * t] = jnp.where(turned & (d < 16), cos, 1.0)
            rope_ref[3 * t + 1] = jnp.where(turned & (d < 8), -sin, 0.0)
            rope_ref[3 * t + 2] = jnp.where(turned & (d >= 8) & (d < 16), sin, 0.0)

    def task_vec():
        vec2 = vec_g[...].reshape(32 * VEC_ROWS, 128).astype(BF16)
        n = iota((1, D), 1).astype(F32)
        spread = dot(vec2, one_hot_cols(24, jnp.broadcast_to(n, (128, D))))
        r = iota((32 * VEC_ROWS, 1), 0).astype(F32)
        mine = floor_div(n, 24) == floor_div(r, VEC_ROWS)
        spread = jnp.where(mine, spread, 0.0).astype(BF16)
        rr = iota((1, 32 * VEC_ROWS), 1).astype(F32)
        kind = rr - floor_div(rr, VEC_ROWS) * VEC_ROWS
        pick = (iota((VEC_ROWS, 32 * VEC_ROWS), 0).astype(F32) == kind).astype(BF16)
        vrow_scr[...] = dot(pick, spread)
        dev = iota((32, 1), 0).astype(F32)

        def long_row(kind, width, cols):
            g = vec_g[0, :, :, :, :, kind].reshape(32, 128).astype(BF16)
            n = cols.astype(F32)
            full = dot(g, one_hot_cols(width, jnp.broadcast_to(n, (128, n.shape[1]))))
            return jnp.sum(jnp.where(floor_div(n, width) == dev, full, 0.0), axis=0, keepdims=True)

        for l in range(2):
            bq_scr[l] = long_row(14 + l, 72, iota((1, 3 * D), 1))
            for zb in range(4):
                bi_scr[l, :, pl.ds(384 * zb, 384)] = long_row(16 + l, 96, iota((1, 384), 1) + (768 * zb + 384 * y))

    def vrow(kind):
        return vrow_scr[pl.ds(kind, 1), :]

    def x_of(l):
        return (x_ref if l == 0 else x1_scr)[...]

    def task_start(l):
        send_x(l).start()
        h1_scr[...] = layer_norm(x_of(l).astype(F32), vrow(l), vrow(2 + l))

    def task_qkv(l, i):
        w = qkv_g[l, :, :, :, :, :, pl.ds(768 * i, 768)].reshape(D, 768)
        got = (dot(h1_scr[...], w) + bq_scr[l, :, pl.ds(768 * i, 768)]).astype(BF16).astype(F32)
        for m in range(2):
            tiles = []
            for t in range(3):
                v = got[:, 384 * m + 128 * t: 384 * m + 128 * t + 128]
                r = v * rope_ref[3 * t] + pltpu.roll(v, 120, 1) * rope_ref[3 * t + 1] + pltpu.roll(v, 8, 1) * rope_ref[3 * t + 2]
                tiles.append(r.astype(BF16).astype(F32))
            h = 4 * i + 2 * m
            t0, t1, t2 = tiles
            q_scr[pl.ds(h, ROWS, stride=16), :] = t0
            kn_scr[pl.ds(h, ROWS, stride=16), :] = pltpu.roll(t0, 64, 1)
            vn_scr[pl.ds(h, ROWS, stride=16), :] = t1
            q_scr[pl.ds(h + 1, ROWS, stride=16), :] = pltpu.roll(t1, 64, 1)
            kn_scr[pl.ds(h + 1, ROWS, stride=16), :] = t2
            vn_scr[pl.ds(h + 1, ROWS, stride=16), :] = pltpu.roll(t2, 64, 1)

    def task_att(l, blk):
        for cp in cache_in(l * BLOCKS + blk):
            cp.wait()
        key = iota((1, KEYS), 1)
        head_row = jnp.minimum(iota((16, 1), 0), HEADS - 1) * SLOTS
        slot_of = key - head_row
        own_head = (slot_of >= 0) & (slot_of < SLOTS)
        slots = iota((SLOTS, HEAD), 0)

        def scores(j):
            b = blk * SEQS + j
            pos = pos_ref[b]
            rows = pl.ds(b * 16, 16)
            put = jnp.where(slots == pos, 1.0, 0.0).astype(BF16) > 0.5

            def placed(buf, new_scr):
                new = new_scr[rows, :][:HEADS, :HEAD].astype(BF16)
                both = jnp.where(put[None], new[:, None, :], buf[l, blk * SEQS + j])
                buf[l, blk * SEQS + j] = both
                return both.reshape(KEYS, HEAD)

            keys = placed(kbuf, kn_scr)
            placed(vbuf, vn_scr)
            q = q_scr[rows, :][:, :HEAD].astype(BF16)
            s = lax.dot_general(q, keys, (((1,), (1,)), ((), ())), preferred_element_type=F32) * (HEAD ** -0.5)
            s_scr[pl.ds(j * 16, 16), :] = jnp.where(own_head & (slot_of <= pos), s, -jnp.inf)

        def weighted(j):
            p = s_scr[pl.ds(j * 16, 16), :].astype(BF16)
            got = dot(p, vbuf[l, blk * SEQS + j].reshape(KEYS, HEAD))
            ctx_scr[pl.ds((blk * SEQS + j) * 16, 16), pl.ds(0, HEAD)] = got

        for j in range(SEQS):
            scores(j)
        s = s_scr[...]
        e = jnp.exp(s - jnp.max(s, axis=-1, keepdims=True))
        s_scr[...] = e / jnp.sum(e, axis=-1, keepdims=True)
        for j in range(SEQS):
            weighted(j)

    def task_h2(l):
        send_x(l).wait_recv()
        for half, v in enumerate((x_of(l), xn_scr[l])):
            h2_scr[pl.ds(ROWS * half, ROWS), :] = layer_norm(v.astype(F32), vrow(4 + l), vrow(6 + l))

    def task_win(l, zb):
        cols = pl.ds(384 * zb, 384)
        w = win_g[l, :, :, :, :, :, cols].reshape(D, 384)
        u = dot(h2_scr[...], w) + bi_scr[l, :, cols]
        act_scr[:, cols] = (0.5 * u * (1.0 + lax.erf(u * 0.7071067811865476))).astype(BF16)

    def task_down(l, i):
        cols = pl.ds(384 * i, 384)
        got = dot(act_scr[...], down_g[l, :, :, :, :, cols].reshape(HID, 384))
        acc_scr[:, cols] = got[:ROWS]
        ps_scr[l, :, cols] = got[ROWS:]
        send_part(l, i).start()

    def task_out(l):
        tiles = []
        for m in range(HEADS // 2):
            a = ctx_scr[pl.ds(2 * m, ROWS, stride=16), :]
            b = pltpu.roll(ctx_scr[pl.ds(2 * m + 1, ROWS, stride=16), :], 64, 1)
            tiles.append(jnp.where(lane < 64, a, b).astype(BF16))
        a = dot(jnp.concatenate(tiles, axis=1), out_g[l].reshape(D, D)) + vrow(8 + l)
        for i in range(2):
            send_part(l, i).wait_recv()
        m = acc_scr[...] + pr_scr[l] + vrow(10 + l)
        new = (x_of(l).astype(F32) + a + m).astype(BF16)
        if l == 0:
            x1_scr[...] = new
        else:
            y_ref[...] = layer_norm(new.astype(F32), vrow(12), vrow(13))

    tasks = {'vec': task_vec}
    for l in range(2):
        tasks[f's{l}'] = functools.partial(task_start, l)
        tasks[f'h{l}'] = functools.partial(task_h2, l)
        tasks[f'o{l}'] = functools.partial(task_out, l)
        for name, fn, count in (('q', task_qkv, 3), ('w', task_win, 4), ('d', task_down, 2), ('a', task_att, BLOCKS)):
            for i in range(count):
                tasks[f'{name}{l}{i}'] = functools.partial(fn, l, i)

    for n, step in enumerate(steps):
        if isinstance(step, str):
            tasks.pop(step)()
            continue
        p, phase = parts[step[0]], step[1]
        if phase < 0:
            for cp in own.pop(specs[step[0]][0] + str(specs[step[0]][1]), ()):
                cp.wait()
        if phase >= 0:
            p.finish(phase)
        if phase + 1 < p.phases:
            p.start(phase + 1)
        if n == FIRST:
            for i in range(2 * BLOCKS):
                for cp in cache_in(i):
                    cp.start()
            task_rope()
    assert not tasks

    for p in parts:
        p.drain()
    for l in range(2):
        send_x(l).wait_send()
        for i in range(2):
            send_part(l, i).wait_send()


def write_kernel(y_ref, k_ref, v_ref, y_hbm, k_hbm, v_hbm, sem):
    copies = [pltpu.make_async_copy(y_ref, y_hbm, sem.at[0])]
    for ref, hbm in ((k_ref, k_hbm), (v_ref, v_hbm)):
        for l in range(2):
            for i in range(4):
                rows = pl.ds(16 * i, 16)
                copies.append(pltpu.make_async_copy(ref.at[l, rows], hbm.at[l, rows], sem.at[len(copies)]))
    for cp in copies:
        cp.start()
    for cp in copies:
        cp.wait()


def fused(pos, x, vecs, w_qkv, w_out, w_in, w_down, k_cache, v_cache):
    specs, steps = make_plan()
    parts = len(specs)
    vmem = pl.BlockSpec(memory_space=pltpu.VMEM)
    hbm = pl.BlockSpec(memory_space=pl.ANY)
    lead = (4, 2, 2, 2)
    dma = pltpu.SemaphoreType.DMA
    outs = (x, k_cache, v_cache)
    y, k_new, v_new = pl.pallas_call(
        functools.partial(kernel, specs, steps),
        out_shape=tuple(pltpu.VMEM(a.shape, a.dtype) for a in outs),
        in_specs=[pl.BlockSpec(memory_space=pltpu.SMEM), vmem] + [vmem] * len(vecs) + [hbm] * 6,
        out_specs=[vmem] * 3,
        scratch_shapes=[
            pltpu.VMEM((1,) + lead + (VEC_ROWS, 128), F32),
            pltpu.VMEM((2,) + lead + (24, 3 * D), BF16),
            pltpu.VMEM((2,) + lead + (24, D), BF16),
            pltpu.VMEM((2,) + lead + (24, HID), BF16),
            pltpu.VMEM((2, 4, 2, 2, 96, D), BF16),
            pltpu.VMEM((ROWS, D), BF16),
            pltpu.VMEM((2, ROWS, D), BF16),
            pltpu.VMEM((2, ROWS, D), F32),
            pltpu.VMEM((2, ROWS, D), F32),
            pltpu.VMEM((ROWS, D), BF16),
            pltpu.VMEM((2 * ROWS, D), BF16),
            pltpu.VMEM((2 * ROWS, HID), BF16),
            pltpu.VMEM((ROWS, D), F32),
            pltpu.VMEM((9, ROWS, 128), F32),
            pltpu.VMEM((ROWS, 128), F32),
            pltpu.VMEM((VEC_ROWS, D), F32),
            pltpu.VMEM((2, 1, 3 * D), F32),
            pltpu.VMEM((2, 1, HID), F32),
            pltpu.VMEM((16 * ROWS, 128), F32),
            pltpu.VMEM((16 * ROWS, 128), F32),
            pltpu.VMEM((16 * ROWS, 128), F32),
            pltpu.VMEM((16 * ROWS, 128), F32),
            pltpu.VMEM((16 * SEQS, KEYS), F32),
            dma((16,)), dma((parts, SENDS)), dma((parts, SENDS)), dma((2,)), dma((2,)), dma((2, 2)), dma((2, 2)), dma((2, 2 * BLOCKS)),
        ],
        compiler_params=pltpu.CompilerParams(collective_id=0, has_side_effects=True, vmem_limit_bytes=VMEM_LIMIT),
    )(pos, x, *vecs, w_qkv, w_out, w_in, w_down, k_cache, v_cache)
    return pl.pallas_call(
        write_kernel,
        out_shape=tuple(jax.ShapeDtypeStruct(a.shape, a.dtype) for a in outs),
        in_specs=[vmem] * 3,
        out_specs=[hbm] * 3,
        scratch_shapes=[dma((17,))],
        compiler_params=pltpu.CompilerParams(vmem_limit_bytes=VMEM_SMALL),
    )(y, k_new, v_new)


def solution(mesh):
    row_spec = P('dp', None)
    vec_spec = P(None, 'dp')
    mat_spec = P(None, 'dp', None)
    cache_spec = P(None, 'dp', None, None, None)
    in_specs = (row_spec, P('dp'), cache_spec, cache_spec, vec_spec, vec_spec, vec_spec, vec_spec, mat_spec, vec_spec, mat_spec, vec_spec, mat_spec, vec_spec, mat_spec, vec_spec, P('dp'), P('dp'))
    out_specs = (row_spec, cache_spec, cache_spec)

    def device_step(x_embed, positions, k_cache, v_cache, ln1_gain, ln1_bias, ln2_gain, ln2_bias, w_qkv, b_qkv, w_out, b_out, w_in, b_in, w_down, b_down, lnf_gain, lnf_bias):
        vecs = (ln1_gain, ln1_bias, ln2_gain, ln2_bias, b_out, b_down, lnf_gain[None], lnf_bias[None], b_qkv, b_in)
        by_head = lambda a: jnp.swapaxes(a, 2, 3)
        out, k_new, v_new = fused(positions, x_embed, vecs, w_qkv, w_out, w_in, w_down, by_head(k_cache), by_head(v_cache))
        return out, by_head(k_new), by_head(v_new)

    return jax.shard_map(device_step, mesh=mesh, in_specs=in_specs, out_specs=out_specs, check_vma=False)
```
